16 devices in a mesh: dp: 4 (over y, z, core), tp: 4 (over x).
Axes of the slice: x: 4, y: 2, z: 1, core: 2. Of those that a mesh axis runs over, the one named last changes fastest.
The devices are a block of a 4x4x8 slice.
Arguments:
- x: bfloat16 [8192, 2048], P(('dp', 'tp')), parts along dimension 0
- dy: bfloat16 [8192, 2048], P(('dp', 'tp')), parts along dimension 0
- gain: bfloat16 [2048], replicated
- wq: bfloat16 [2048, 3072], P(None, 'tp')
- wk: bfloat16 [2048, 3072], P(None, 'tp')
- wv: bfloat16 [2048, 3072], P(None, 'tp')
- wo: bfloat16 [3072, 2048], P('tp')
Outputs:
- output 1: bfloat16 [8192, 2048], P(('dp', 'tp')), parts along dimension 0
- output 2: float32 [4, 2048], P('dp'), parts along dimension 0
- output 3: bfloat16 [8192, 3072], P('dp', 'tp'), parts along dimension 0
- output 4: bfloat16 [8192, 3072], P('dp', 'tp'), parts along dimension 0
- output 5: bfloat16 [8192, 3072], P('dp', 'tp'), parts along dimension 0
- output 6: bfloat16 [12288, 2048], P(('dp', 'tp')), parts along dimension 0
There are 4 independent parts. The reference program is written for one: setup_inputs(seed, part) draws one part's arguments, and reference() takes and returns one part's arrays. A program takes and returns all parts, laid end to end along the dimension named above; an argument that names none is the same for every part.
All inputs are finite; a program needn't handle non-finite values.
Results may differ from the reference program's by a relative error of at most 0.018.
Values are sent between devices in bfloat16 or wider.
A program may use at most 768 MiB of HBM per device.

```python
import jax
import jax.numpy as jnp
from jax import lax

ROWS = 2048
D = 2048
HEADS = 24
KV_HEADS = 24
HEAD = 128
THETA = 10000


def setup_inputs(seed: int = 0, part: int = 0) -> dict:
    kx, ky, kn, kq, kk, kv, ko = jax.random.split(jax.random.key(seed), 7)

    def weights(key, rows, columns):
        return jax.random.normal(key, (rows, columns), jnp.float32) * rows**-0.5

    drawn = {
        "x": jax.random.normal(jax.random.fold_in(kx, part), (ROWS, D), jnp.float32),
        "dy": jax.random.normal(jax.random.fold_in(ky, part), (ROWS, D), jnp.float32) * ROWS**-0.5,
        "gain": 1 + 0.1 * jax.random.normal(kn, (D,), jnp.float32),
        "wq": 2 * weights(kq, D, HEADS * HEAD),
        "wk": 2 * weights(kk, D, KV_HEADS * HEAD),
        "wv": 4 * weights(kv, D, KV_HEADS * HEAD),
        "wo": weights(ko, HEADS * HEAD, D),
    }
    return {k: v.astype(jnp.bfloat16) for k, v in drawn.items()}


def normed(x, gain):
    wide = x.astype(jnp.float32)
    scale = lax.rsqrt(jnp.mean(wide * wide, -1, keepdims=True) + 1e-6)
    return (wide * scale * gain.astype(jnp.float32)).astype(jnp.bfloat16)


def turned(t, place, theta):
    half = t.shape[-1] // 2
    angle = place.astype(jnp.float32)[:, None] * theta ** (-jnp.arange(half, dtype=jnp.float32) / half)
    cos, sin = jnp.cos(angle)[:, None], jnp.sin(angle)[:, None]
    a, b = t[..., :half].astype(jnp.float32), t[..., half:].astype(jnp.float32)
    return jnp.concatenate([a * cos - b * sin, b * cos + a * sin], -1).astype(jnp.bfloat16)


def matmul(a, w):
    return jnp.dot(a, w, preferred_element_type=jnp.float32).astype(jnp.bfloat16)


def einsum(form, a, b):
    return jnp.einsum(form, a.astype(jnp.float32), b.astype(jnp.float32))


def attention(q, k, v):
    scores = einsum("tgsd,ugd->gstu", q, k) * q.shape[-1] ** -0.5
    token = jnp.arange(q.shape[0])
    scores = jnp.where(token[:, None] >= token, scores, -jnp.inf)
    weights = jax.nn.softmax(scores, -1).astype(jnp.bfloat16)
    return einsum("gstu,ugd->tgsd", weights, v).astype(jnp.bfloat16)


def forward(x, gain, wq, wk, wv, wo):
    rows = x.shape[0]
    a, place = normed(x, gain), jnp.arange(rows)
    k = turned(matmul(a, wk).reshape(rows, -1, HEAD), place, THETA)
    q = turned(matmul(a, wq).reshape(rows, -1, HEAD), place, THETA).reshape(rows, k.shape[1], -1, HEAD)
    v = matmul(a, wv).reshape(rows, -1, HEAD)
    seen = attention(q, k, v).reshape(rows, -1)
    return (x.astype(jnp.float32) + jnp.dot(seen, wo, preferred_element_type=jnp.float32)).astype(jnp.bfloat16)


def reference(x, dy, gain, wq, wk, wv, wo):
    _, back = jax.vjp(forward, x, gain.astype(jnp.float32), wq, wk, wv, wo)
    by_x, by_gain, *by_weights = back(dy)
    return (by_x, by_gain[None], *by_weights)
```

```python
import functools

import jax
import jax.numpy as jnp
from jax import lax
from jax.experimental import pallas as pl
from jax.experimental.pallas import tpu as pltpu
from jax.sharding import PartitionSpec as P

HEAD = 128
THETA = 10000
NEG = -1e30
HIDDEN = 2 * NEG
LOG2E = 1.4426950408889634
VMEM = 58 * 2**20
LOW = jnp.bfloat16
WIDE = jnp.float32


def _dot(a, b, ca, cb):
    return lax.dot_general(a, b, (((ca,), (cb,)), ((), ())), preferred_element_type=WIDE)


def _params(**more):
    return pltpu.CompilerParams(vmem_limit_bytes=VMEM, **more)


def _cost(flops, arrays, exps=0):
    return pl.CostEstimate(flops=int(flops), transcendentals=int(exps), bytes_accessed=int(sum(a.size * a.dtype.itemsize for a in arrays)))


def _like(shape, dtype=LOW):
    return jax.ShapeDtypeStruct(shape, dtype)


ANY = pl.BlockSpec(memory_space=pl.ANY)


def _full(shape):
    return pl.BlockSpec(shape, lambda *_: (0,) * len(shape))


def _turn(t, cos, sin):
    return t * cos + pltpu.roll(t, HEAD // 2, 1) * sin


def _project(*refs):
    top, low, gain, cos, sin, wq, wk, wv = refs[:8]
    a_o, q_o, k_o, v_o, w_s, sem = refs[-6:]
    loads = [pltpu.make_async_copy(w, w_s.at[i], sem.at[i]) for i, w in enumerate((wq, wk, wv))]
    for load in loads:
        load.start()
    half = top.shape[0]
    g = gain[...].astype(WIDE)
    for p, x in enumerate((top, low)):
        wide = x[...].astype(WIDE)
        scale = lax.rsqrt(jnp.mean(wide * wide, -1, keepdims=True) + 1e-6)
        a_o[p * half : (p + 1) * half, :] = (wide * scale * g).astype(LOW)
    for i, out in enumerate((q_o, k_o, v_o)):
        loads[i].wait()
        for at in range(0, out.shape[1], 256):
            t = _dot(a_o[...], w_s[i, :, at : at + 256], 1, 0).astype(LOW)
            if i < 2:
                for h in range(0, 256, HEAD):
                    out[:, at + h : at + h + HEAD] = _turn(t[:, h : h + HEAD].astype(WIDE), cos[...], sin[...]).astype(LOW)
            else:
                out[:, at : at + 256] = t


def project(slot, slots, x, gain, cos, sin, w, kept):
    rows, d = 2 * x[0].shape[0], x[0].shape[1]
    wide = w[0].shape[1]
    at = lambda *_: (slot, 0)
    outs = [_like((slots * rows, n)) for n in (d, wide, wide, wide)]
    given = [*x, gain, cos, sin, *w]
    specs = [_full(x[0].shape)] * 2 + [_full(gain.shape)] + [pl.BlockSpec((rows, HEAD), at)] * 2 + [ANY] * 3
    alias = {}
    if kept is not None:
        alias = {len(given) + i: i for i in range(4)}
        given += kept
        specs += [ANY] * 4
    return pl.pallas_call(
        _project,
        grid=(1,),
        in_specs=specs,
        out_specs=[pl.BlockSpec((rows, n), at) for n in (d, wide, wide, wide)],
        out_shape=outs,
        scratch_shapes=[pltpu.VMEM((3, d, wide), LOW), pltpu.SemaphoreType.DMA((3,))],
        input_output_aliases=alias,
        compiler_params=_params(),
        cost_estimate=_cost(2 * rows * d * 3 * wide, [*x, *w]),
        name=f"project{slot}",
    )(*given)


def _by_seen(*refs):
    top, low, wo = refs[:3]
    dy_o, do_o, w_s, sem = refs[-4:]
    load = pltpu.make_async_copy(wo, w_s, sem)
    load.start()
    half = top.shape[0]
    dy_o[:half, :] = top[...]
    dy_o[half:, :] = low[...]
    load.wait()
    for at in range(0, do_o.shape[1], 256):
        do_o[:, at : at + 256] = _dot(dy_o[...], w_s[at : at + 256, :], 1, 1).astype(LOW)


def by_seen(slot, slots, dy, wo, kept):
    rows, d = 2 * dy[0].shape[0], dy[0].shape[1]
    wide = wo.shape[0]
    at = lambda *_: (slot, 0)
    given, specs, alias = [*dy, wo], [_full(dy[0].shape)] * 2 + [ANY], {}
    if kept is not None:
        alias = {len(given) + i: i for i in range(2)}
        given += kept
        specs += [ANY] * 2
    return pl.pallas_call(
        _by_seen,
        grid=(1,),
        in_specs=specs,
        out_specs=[pl.BlockSpec((rows, n), at) for n in (d, wide)],
        out_shape=[_like((slots * rows, n)) for n in (d, wide)],
        scratch_shapes=[pltpu.VMEM((wide, d), LOW), pltpu.SemaphoreType.DMA],
        input_output_aliases=alias,
        compiler_params=_params(),
        cost_estimate=_cost(2 * rows * d * wide, [*dy, wo]),
        name=f"by_seen{slot}",
    )(*given)


def _slot(block, me, slots):
    return lax.rem(block - me + slots, slots)


def _gap(keys, queries):
    return lax.broadcasted_iota(jnp.int32, (keys, queries), 1) - lax.broadcasted_iota(jnp.int32, (keys, queries), 0)


def _forward(me_ref, q_ref, k_ref, v_ref, o_ref, lse_ref, top_s, mix_s, gap_s, *, slots):
    rows, heads = q_ref.shape[0], q_ref.shape[1] // HEAD
    iq, me = pl.program_id(0), me_ref[0]
    e = HEAD**-0.5 * LOG2E

    @pl.when(iq == 0)
    def _():
        gap_s[...] = _gap(rows, rows)

    top_s[...] = jnp.full_like(top_s, NEG)
    mix_s[...] = jnp.zeros_like(mix_s)
    ones = jnp.ones((8, rows), LOW)
    cut = [slice(h * HEAD, (h + 1) * HEAD) for h in range(heads)]

    def block(j, masked):
        here = pl.ds(_slot(j, me, slots) * rows, rows)
        scores = [_dot(k_ref[here, c], q_ref[:, c], 1, 1) for c in cut]
        weights, keeps = [], []
        for h, s in enumerate(scores):
            if masked:
                s = jnp.where(gap_s[...] >= 0, s, HIDDEN)
            old = top_s[h : h + 1, :]
            top = jnp.maximum(old, s.max(axis=0, keepdims=True))
            top_s[h : h + 1, :] = top
            weights.append(jnp.exp2((s - top) * e).astype(LOW))
            keeps.append(jnp.exp2((old - top) * e))
        for h, (p, keep) in enumerate(zip(weights, keeps)):
            values = jnp.concatenate([v_ref[here, cut[h]].T, ones], axis=0)
            mix_s[h] = mix_s[h] * keep + _dot(values, p, 1, 0)

    lax.fori_loop(0, iq, lambda j, _: block(j, False), None)
    block(iq, True)
    for h in range(heads):
        total = mix_s[h, HEAD : HEAD + 1, :]
        o_ref[:, cut[h]] = (mix_s[h, :HEAD, :] * (1 / total)).T.astype(LOW)
        lse_ref[h : h + 1, :] = top_s[h : h + 1, :] * HEAD**-0.5 + jnp.log(total)


def attend(me, q, k, v, slots):
    total, wide = q.shape
    rows, heads = total // slots, wide // HEAD
    at = lambda i, me_ref: (_slot(i, me_ref[0], slots), 0)
    return pl.pallas_call(
        functools.partial(_forward, slots=slots),
        grid_spec=pltpu.PrefetchScalarGridSpec(
            num_scalar_prefetch=1,
            grid=(slots,),
            in_specs=[pl.BlockSpec((rows, wide), at), _full((total, wide)), _full((total, wide))],
            out_specs=[pl.BlockSpec((rows, wide), at), pl.BlockSpec((heads, rows), lambda i, me_ref: (0, _slot(i, me_ref[0], slots)))],
            scratch_shapes=[pltpu.VMEM((heads, rows), WIDE), pltpu.VMEM((heads, HEAD + 8, rows), WIDE), pltpu.VMEM((rows, rows), jnp.int32)],
        ),
        out_shape=[_like((total, wide)), _like((heads, total), WIDE)],
        compiler_params=_params(),
        cost_estimate=_cost(4 * total * total * wide, [q, k, v, q], total * total * heads),
        name="attend",
    )(me, q, k, v)


def _backward(me_ref, q_ref, k_ref, v_ref, do_ref, o_ref, lse_ref, cosq, sinq, cosk, sink, dq_ref, dk_ref, dv_ref,
              dq_s, dk_s, dv_s, gap_s, *, slots):
    rows, heads = q_ref.shape[0], q_ref.shape[1] // HEAD
    g, iq, me = pl.program_id(0), pl.program_id(1), me_ref[0]
    scale = HEAD**-0.5
    e = scale * LOG2E

    @pl.when(iq == 0)
    def _():
        gap_s[...] = _gap(rows, rows)
        dk_s[...] = jnp.zeros_like(dk_s)
        dv_s[...] = jnp.zeros_like(dv_s)

    dq_s[...] = jnp.zeros_like(dq_s)
    cut = [slice(h * HEAD, (h + 1) * HEAD) for h in range(heads)]
    lses = [lse_ref[0, h : h + 1, :] * LOG2E for h in range(heads)]
    deltas = [(do_ref[:, c].astype(WIDE) * o_ref[:, c].astype(WIDE)).T.sum(axis=0, keepdims=True) for c in cut]

    def block(j, masked):
        here = pl.ds(_slot(j, me, slots) * rows, rows)
        scores = [_dot(k_ref[here, c], q_ref[:, c], 1, 1) for c in cut]
        dps = [_dot(v_ref[here, c], do_ref[:, c], 1, 1) for c in cut]
        for h, c in enumerate(cut):
            p = jnp.exp2(scores[h] * e - lses[h])
            if masked:
                p = jnp.where(gap_s[...] >= 0, p, 0.0)
            ds = (p * (dps[h] - deltas[h])).astype(LOW)
            dv_s[here, c] += _dot(p.astype(LOW), do_ref[:, c], 1, 0)
            dk_s[here, c] += _dot(ds, q_ref[:, c], 1, 0)
            dq_s[h] += _dot(k_ref[here, c].T, ds, 1, 0)

    lax.fori_loop(0, iq, lambda j, _: block(j, False), None)
    block(iq, True)
    for h, c in enumerate(cut):
        dq = (dq_s[h] * scale).T.astype(LOW).astype(WIDE)
        dq_ref[:, c] = _turn(dq, cosq[...], -sinq[...]).astype(LOW)

    @pl.when(iq == pl.num_programs(1) - 1)
    def _():
        for c in cut:
            dk = (dk_s[:, c] * scale).astype(LOW).astype(WIDE)
            dk_ref[:, c] = _turn(dk, cosk[...], -sink[...]).astype(LOW)
            dv_ref[:, c] = dv_s[:, c].astype(LOW)


def attend_bwd(me, q, k, v, do, o, lse, cos, sin, slots, heads=3):
    total, wide = q.shape
    rows, parts = total // slots, wide // HEAD // heads
    width = heads * HEAD
    at = lambda g, i, me_ref: (_slot(i, me_ref[0], slots), g)
    queries = pl.BlockSpec((rows, width), at)
    keys = pl.BlockSpec((total, width), lambda g, i, me_ref: (0, g))
    lse = lse.reshape(parts, heads, total)
    return pl.pallas_call(
        functools.partial(_backward, slots=slots),
        grid_spec=pltpu.PrefetchScalarGridSpec(
            num_scalar_prefetch=1,
            grid=(parts, slots),
            in_specs=[queries, keys, keys, queries, queries,
                      pl.BlockSpec((1, heads, rows), lambda g, i, me_ref: (g, 0, _slot(i, me_ref[0], slots)))]
            + [pl.BlockSpec((rows, HEAD), lambda g, i, me_ref: (_slot(i, me_ref[0], slots), 0))] * 2 + [_full((total, HEAD))] * 2,
            out_specs=[queries, keys, keys],
            scratch_shapes=[pltpu.VMEM((heads, HEAD, rows), WIDE), pltpu.VMEM((total, width), WIDE), pltpu.VMEM((total, width), WIDE),
                            pltpu.VMEM((rows, rows), jnp.int32)],
        ),
        out_shape=[_like((total, wide))] * 3,
        compiler_params=_params(),
        cost_estimate=_cost(10 * total * total * wide, [q] * 8, total * total * wide // HEAD),
        name="attend_bwd",
    )(me, q, k, v, do, o, lse, cos, sin, cos, sin)


def _by_normed(*refs, adds):
    dq, dk, dv, wq, wk, wv = refs[:6]
    out = refs[-1]
    for at in range(0, out.shape[1], 256):
        c = slice(at, at + 256)
        t = _dot(dq[...], wq[c, :], 1, 1) + _dot(dk[...], wk[c, :], 1, 1) + _dot(dv[...], wv[c, :], 1, 1)
        for more in refs[6 : 6 + adds]:
            t += more[:, c].astype(WIDE)
        out[:, c] = t.astype(out.dtype)


def by_normed(slot, slots, dqkv, w, first, columns, adds=(), dtype=LOW, tile=512):
    rows, wide = dqkv[0].shape[0] // slots, dqkv[0].shape[1]
    base = first // tile
    return pl.pallas_call(
        functools.partial(_by_normed, adds=len(adds)),
        grid=(columns // tile,),
        in_specs=[pl.BlockSpec((rows, wide), lambda i: (slot, 0))] * 3 + [pl.BlockSpec((tile, wide), lambda i: (base + i, 0))] * 3
        + [pl.BlockSpec((rows, tile), lambda i: (0, i))] * len(adds),
        out_specs=pl.BlockSpec((rows, tile), lambda i: (0, i)),
        out_shape=_like((rows, columns), dtype),
        compiler_params=_params(),
        cost_estimate=_cost(2 * rows * columns * 3 * wide, [*w, *adds]),
        name=f"by_normed{slot}_{first}",
    )(*dqkv, *w, *adds)


def _finish(t, la, lb, ra, rb, x_ref, dy, gain, dx_o, dg_o):
    half = la.shape[1]
    x = x_ref[...].astype(WIDE)
    d = x.shape[1]
    dn = jnp.concatenate([t[:, :half] + la[...].astype(WIDE) + ra[...].astype(WIDE), t[:, half:] + lb[...].astype(WIDE) + rb[...].astype(WIDE)], 1)
    scale = lax.rsqrt(jnp.mean(x * x, -1, keepdims=True) + 1e-6)
    there = x * scale

    @pl.when(pl.program_id(0) == 0)
    def _():
        dg_o[...] = jnp.zeros_like(dg_o)

    dg_o[...] += (dn * there).reshape(-1, 8, d).sum(0)
    dh = dn * gain[...].astype(WIDE)
    dx = scale * (dh - there * jnp.mean(dh * there, -1, keepdims=True))
    dx_o[...] = (dx + dy[...].astype(WIDE)).astype(LOW)


def finish(t, la, lb, ra, rb, x, dy, gain, step=128):
    rows, d = x.shape
    full, half = pl.BlockSpec((step, d), lambda i: (i, 0)), pl.BlockSpec((step, d // 2), lambda i: (i, 0))
    return pl.pallas_call(
        _finish,
        grid=(rows // step,),
        in_specs=[full, half, half, half, half, full, full, _full(gain.shape)],
        out_specs=[full, _full((8, d))],
        out_shape=[_like((rows, d)), _like((8, d), WIDE)],
        compiler_params=_params(),
        cost_estimate=_cost(20 * rows * d, [t, x, x, x, x, x]),
        name="finish",
    )(t, la, lb, ra, rb, x, dy, gain)


def solution(mesh):
    slots = mesh.shape["tp"]
    right = [(i, (i + 1) % slots) for i in range(slots)]
    left = [(i, (i - 1) % slots) for i in range(slots)]

    def send(t, ring):
        return lax.ppermute(t, "tp", ring)

    def gather(t):
        half = t.shape[0] // 2
        top, low = t[:half], t[half:]
        from_left_top, from_right_low = send(top, right), send(low, left)
        from_left_low, from_right_top = send(low, right), send(top, left)
        far_top, far_low = send(from_left_top, right), send(from_right_low, left)
        return [(top, low), (from_right_top, from_right_low), (far_top, far_low), (from_left_top, from_left_low)]

    def step(x, dy, gain, wq, wk, wv, wo):
        rows, d = x.shape
        total = slots * rows
        w = (wq, wk, wv)
        me = lax.axis_index("tp")
        me_s = me.astype(jnp.int32)[None]
        gain_row = gain[None]
        place = jnp.concatenate([lax.rem(me + s, slots) * rows + jnp.arange(rows) for s in range(slots)])
        half = HEAD // 2
        angle = place.astype(WIDE)[:, None] * THETA ** (-jnp.arange(half, dtype=WIDE) / half)
        c, s = jnp.cos(angle), jnp.sin(angle)
        cos, sin = jnp.concatenate([c, c], 1), jnp.concatenate([-s, s], 1)

        xs = gather(x)
        dy_then, _ = lax.optimization_barrier((dy, (xs[3][1], xs[1][0])))
        dys = gather(dy_then)

        kept, grads = None, None
        for slot in (0, 1, 3, 2):
            kept = project(slot, slots, xs[slot], gain_row, cos, sin, w, kept)
        a, q, k, v = kept
        o, lse = attend(me_s, q, k, v, slots)
        for slot in (0, 1, 3, 2):
            grads = by_seen(slot, slots, dys[slot], wo, grads)
        dy_all, do = grads
        dqkv = attend_bwd(me_s, q, k, v, do, o, lse, cos, sin, slots)

        part = functools.partial(by_normed, slots=slots, dqkv=dqkv, w=w, columns=d // 2)
        far_a = send(part(2, first=0), right)
        far_b = send(part(2, first=d // 2), left)
        from_left_b = send(part(1, first=d // 2), right)
        from_right_a = send(part(3, first=0), left)
        from_left_a = send(part(1, first=0, adds=(far_a,)), right)
        from_right_b = send(part(3, first=d // 2, adds=(far_b,)), left)
        own = by_normed(0, slots, dqkv, w, 0, d, dtype=WIDE)
        by_w = [lax.dot_general(a, t, (((0,), (0,)), ((), ())), preferred_element_type=WIDE).astype(LOW) for t in dqkv]
        by_wo = lax.dot_general(o, dy_all, (((0,), (0,)), ((), ())), preferred_element_type=WIDE).astype(LOW)
        by_x, by_gain = finish(own, from_left_a, from_left_b, from_right_a, from_right_b, x, dy, gain_row)
        by_gain = lax.psum(by_gain.sum(0)[None], "tp")
        return (by_x, by_gain, *by_w, by_wo)

    tokens, columns = P(("dp", "tp"), None), P(None, "tp")
    return jax.shard_map(
        step,
        mesh=mesh,
        in_specs=(tokens, tokens, P(None), columns, columns, columns, P("tp", None)),
        out_specs=(tokens, P("dp", None), P("dp", "tp"), P("dp", "tp"), P("dp", "tp"), P(("dp", "tp"), None)),
        check_vma=False,
    )
```

```python
import functools

import jax
import jax.numpy as jnp
from jax import lax
from jax.experimental import pallas as pl
from jax.experimental.pallas import tpu as pltpu
from jax.sharding import PartitionSpec as P

HEAD = 128
THETA = 10000
NEG = -1e30
HIDDEN = 2 * NEG
LOG2E = 1.4426950408889634
VMEM = 58 * 2**20
LOW = jnp.bfloat16
WIDE = jnp.float32


def _dot(a, b, ca, cb):
    return lax.dot_general(a, b, (((ca,), (cb,)), ((), ())), preferred_element_type=WIDE)


def _params(**more):
    return pltpu.CompilerParams(vmem_limit_bytes=VMEM, **more)


def _cost(flops, arrays, exps=0):
    return pl.CostEstimate(flops=int(flops), transcendentals=int(exps), bytes_accessed=int(sum(a.size * a.dtype.itemsize for a in arrays)))


def _like(shape, dtype=LOW):
    return jax.ShapeDtypeStruct(shape, dtype)


ANY = pl.BlockSpec(memory_space=pl.ANY)


def _full(shape):
    return pl.BlockSpec(shape, lambda *_: (0,) * len(shape))


def _turn(t, cos, sin):
    return t * cos + pltpu.roll(t, HEAD // 2, 1) * sin


def _slot(block, me, slots):
    return lax.rem(block - me + slots, slots)


def _gap(keys, queries):
    return lax.broadcasted_iota(jnp.int32, (keys, queries), 1) - lax.broadcasted_iota(jnp.int32, (keys, queries), 0)


def _attend(iq, me, slots, rows, heads, qkv_s, o_s, lse_o, top_s, mix_s, gap_s):
    wide = heads * HEAD
    e = HEAD**-0.5 * LOG2E
    mine = pl.ds(_slot(iq, me, slots) * rows, rows)
    top_s[...] = jnp.full_like(top_s, NEG)
    mix_s[...] = jnp.zeros_like(mix_s)
    ones = jnp.ones((8, rows), LOW)
    cut = [slice(h * HEAD, (h + 1) * HEAD) for h in range(3 * heads)]

    def block(j, masked):
        here = pl.ds(_slot(j, me, slots) * rows, rows)
        scores = [_dot(qkv_s[here, cut[heads + h]], qkv_s[mine, cut[h]], 1, 1) for h in range(heads)]
        weights, keeps = [], []
        for h, s in enumerate(scores):
            if masked:
                s = jnp.where(gap_s[...] >= 0, s, HIDDEN)
            old = top_s[h : h + 1, :]
            top = jnp.maximum(old, s.max(axis=0, keepdims=True))
            top_s[h : h + 1, :] = top
            weights.append(jnp.exp2((s - top) * e).astype(LOW))
            keeps.append(jnp.exp2((old - top) * e))
        for h, (p, keep) in enumerate(zip(weights, keeps)):
            values = jnp.concatenate([qkv_s[here, cut[2 * heads + h]].T, ones], axis=0)
            mix_s[h] = mix_s[h] * keep + _dot(values, p, 1, 0)

    lax.fori_loop(0, iq, lambda j, _: block(j, False), None)
    block(iq, True)
    for h in range(heads):
        total = mix_s[h, HEAD : HEAD + 1, :]
        o_s[mine, cut[h]] = (mix_s[h, :HEAD, :] * (1 / total)).T.astype(LOW)
        lse_o[_slot(iq, me, slots), h : h + 1, :] = top_s[h : h + 1, :] * HEAD**-0.5 + jnp.log(total)


def _front(x, dy, gain, cos, sin, wq, wk, wv, wo, xs, dys, a_o, qkv_o, o_o, do_o, lse_o,
           w_s, wo_s, x_s, a_s, qkv_s, o_s, do_s, top_s, mix_s, gap_s, w_sem, x_sem, a_sem, out_sem, send_sem, recv_sem, *, slots):
    me = lax.axis_index("tp")
    rows, d = x.shape
    half, wide = rows // 2, wq.shape[1]
    heads = wide // HEAD
    right, left = lax.rem(me + 1, slots), lax.rem(me + slots - 1, slots)
    top, low = pl.ds(0, half), pl.ds(half, half)
    last = slots - 1

    barrier = pltpu.get_barrier_semaphore()
    for there in (left, right):
        pl.semaphore_signal(barrier, inc=1, device_id={"tp": there}, device_id_type=pl.DeviceIdType.MESH)
    pl.semaphore_wait(barrier, 2)

    def send(n, src, dst, there):
        copy = pltpu.make_async_remote_copy(src_ref=src, dst_ref=dst, send_sem=send_sem.at[n], recv_sem=recv_sem.at[n],
                                            device_id={"tp": there}, device_id_type=pl.DeviceIdType.MESH)
        copy.start()
        return copy

    def near(n, t, ts):
        return [send(n, t.at[top], ts.at[last, 0], right), send(n + 1, t.at[low], ts.at[1, 1], left),
                send(n + 2, t.at[low], ts.at[last, 1], right), send(n + 3, t.at[top], ts.at[1, 0], left)]

    def far(n, ts):
        return [send(n, ts.at[last, 0], ts.at[2, 0], right), send(n + 1, ts.at[1, 1], ts.at[2, 1], left)]

    x_near = near(0, x, xs)

    def load(src, dst, sem):
        copy = pltpu.make_async_copy(src, dst, sem)
        copy.start()
        return copy

    def block(t, ts, slot):
        if slot == 0:
            return [load(t, x_s, x_sem.at[0])]
        return [load(ts.at[slot, p], x_s.at[pl.ds(p * half, half)], x_sem.at[p]) for p in range(2)]

    loads = block(x, xs, 0)
    w_loads = [load(w, w_s.at[:, pl.ds(i * wide, wide)], w_sem.at[i]) for i, w in enumerate((wq, wk, wv))]
    wo_load = load(wo, wo_s, w_sem.at[3])
    gap_s[...] = _gap(rows, rows)
    g = gain[...].astype(WIDE)
    outs = []

    def normed(slot):
        for p in range(0, rows, 128):
            t = x_s[p : p + 128, :].astype(WIDE)
            scale = lax.rsqrt(jnp.mean(t * t, -1, keepdims=True) + 1e-6)
            a_s[p : p + 128, :] = (t * scale * g).astype(LOW)
        outs.append(load(a_s, a_o.at[pl.ds(slot * rows, rows)], a_sem.at[slot]))

    def project(slot):
        at = slice(slot * rows, (slot + 1) * rows)
        def turned(i, _):
            c = pl.ds(pl.multiple_of(i * 256, 256), 256)
            t = _dot(a_s[...], w_s[:, c], 1, 0).astype(LOW).astype(WIDE)
            qkv_s[at, c] = jnp.concatenate([_turn(t[:, h : h + HEAD], cos[at, :], sin[at, :]) for h in (0, HEAD)], 1).astype(LOW)
        def plain(i, _):
            c = pl.ds(pl.multiple_of(i * 256, 256), 256)
            qkv_s[at, c] = _dot(a_s[...], w_s[:, c], 1, 0).astype(LOW)
        lax.fori_loop(0, 2 * wide // 256, turned, None)
        lax.fori_loop(2 * wide // 256, 3 * wide // 256, plain, None)
        outs.append(load(qkv_s.at[pl.ds(slot * rows, rows)], qkv_o.at[pl.ds(slot * rows, rows)], out_sem.at[slot]))

    def by_seen(slot):
        at = slice(slot * rows, (slot + 1) * rows)
        for c in range(0, wide, 256):
            do_s[at, c : c + 256] = _dot(x_s[...], wo_s[c : c + 256, :], 1, 1).astype(LOW)
        outs.append(load(do_s.at[pl.ds(slot * rows, rows)], do_o.at[pl.ds(slot * rows, rows)], out_sem.at[slots + slot]))

    def wait(copies):
        for copy in copies:
            copy.wait()

    wait(loads)
    normed(0)
    wait(w_loads)
    loads = block(dy, dys, 0)
    project(0)
    wait(loads)
    keep = load(x_s.at[top], dys.at[0, 0], x_sem.at[0]), load(x_s.at[low], dys.at[0, 1], x_sem.at[1])
    wo_load.wait()
    by_seen(0)
    wait(keep)
    x_near[0].wait_recv()
    x_near[1].wait_recv()
    x_far = far(4, xs)
    x_near[3].wait_recv()
    loads = block(x, xs, 1)
    x_near[2].wait_recv()
    dy_near = near(6, dy, dys)
    for slot in (1, last):
        wait(loads)
        outs[-3 if slot == 1 else -2].wait()
        outs.pop(-3 if slot == 1 else -2)
        normed(slot)
        if slot == 1:
            loads = block(x, xs, last)
        project(slot)
    x_far[0].wait_recv()
    x_far[1].wait_recv()
    wait(block(x, xs, 2))
    outs[-2].wait()
    outs.pop(-2)
    normed(2)
    project(2)

    def attend(iq, _):
        _attend(iq, me, slots, rows, heads, qkv_s, o_s, lse_o, top_s, mix_s, gap_s)

    lax.fori_loop(0, slots, attend, None)
    dy_near[0].wait_recv()
    dy_near[1].wait_recv()
    dy_far = far(10, dys)
    outs.append(load(o_s, o_o, out_sem.at[2 * slots]))
    dy_near[3].wait_recv()
    wait(block(dy, dys, 1))
    by_seen(1)
    dy_near[2].wait_recv()
    wait(block(dy, dys, last))
    by_seen(last)
    dy_far[0].wait_recv()
    dy_far[1].wait_recv()
    wait(block(dy, dys, 2))
    by_seen(2)
    wait(outs)
    for copy in (*x_near, *x_far, *dy_near, *dy_far):
        copy.wait_send()


def front(x, dy, gain, cos, sin, wq, wk, wv, wo, slots):
    rows, d = x.shape
    wide = wq.shape[1]
    total, heads = slots * rows, wide // HEAD
    blocks = _like((slots, 2, rows // 2, d))
    copies = pltpu.SemaphoreType.DMA((12,))
    return pl.pallas_call(
        functools.partial(_front, slots=slots),
        in_specs=[ANY, ANY] + [pl.BlockSpec(memory_space=pltpu.VMEM)] * 3 + [ANY] * 4,
        out_specs=[ANY] * 6 + [pl.BlockSpec(memory_space=pltpu.VMEM)],
        out_shape=[blocks, blocks, _like((total, d)), _like((total, 3 * wide)), _like((total, wide)), _like((total, wide)),
                   _like((slots, heads, rows), WIDE)],
        scratch_shapes=[pltpu.VMEM((d, 3 * wide), LOW), pltpu.VMEM((wide, d), LOW), pltpu.VMEM((rows, d), LOW), pltpu.VMEM((rows, d), LOW),
                        pltpu.VMEM((total, 3 * wide), LOW), pltpu.VMEM((total, wide), LOW), pltpu.VMEM((total, wide), LOW),
                        pltpu.VMEM((heads, rows), WIDE), pltpu.VMEM((heads, HEAD + 8, rows), WIDE), pltpu.VMEM((rows, rows), jnp.int32),
                        pltpu.SemaphoreType.DMA((4,)), pltpu.SemaphoreType.DMA((2,)), pltpu.SemaphoreType.DMA((slots,)),
                        pltpu.SemaphoreType.DMA((2 * slots + 1,)), copies, copies],
        compiler_params=_params(collective_id=0, has_side_effects=True),
        cost_estimate=_cost(2 * total * d * 4 * wide + 4 * total * total * wide, [x] * 20, total * total * heads),
        name="front",
    )(x, dy, gain, cos, sin, wq, wk, wv, wo)


def _backward(me_ref, q_ref, k_ref, v_ref, do_ref, o_ref, lse_ref, cosq, sinq, cosk, sink, dq_ref, dk_ref, dv_ref,
              dq_s, dk_s, dv_s, gap_s, *, slots):
    rows, heads = q_ref.shape[0], q_ref.shape[1] // HEAD
    g, iq, me = pl.program_id(0), pl.program_id(1), me_ref[0]
    scale = HEAD**-0.5
    e = scale * LOG2E

    @pl.when(iq == 0)
    def _():
        gap_s[...] = _gap(rows, rows)
        dk_s[...] = jnp.zeros_like(dk_s)
        dv_s[...] = jnp.zeros_like(dv_s)

    dq_s[...] = jnp.zeros_like(dq_s)
    cut = [slice(h * HEAD, (h + 1) * HEAD) for h in range(heads)]
    lses = [lse_ref[0, pl.ds(g * heads + h, 1), :] * LOG2E for h in range(heads)]
    deltas = [(do_ref[:, c].astype(WIDE) * o_ref[:, c].astype(WIDE)).T.sum(axis=0, keepdims=True) for c in cut]

    def block(j, masked):
        here = pl.ds(_slot(j, me, slots) * rows, rows)
        scores = [_dot(k_ref[here, c], q_ref[:, c], 1, 1) for c in cut]
        dps = [_dot(v_ref[here, c], do_ref[:, c], 1, 1) for c in cut]
        for h, c in enumerate(cut):
            p = jnp.exp2(scores[h] * e - lses[h])
            if masked:
                p = jnp.where(gap_s[...] >= 0, p, 0.0)
            ds = (p * (dps[h] - deltas[h])).astype(LOW)
            dv_s[here, c] += _dot(p.astype(LOW), do_ref[:, c], 1, 0)
            dk_s[here, c] += _dot(ds, q_ref[:, c], 1, 0)
            dq_s[h] += _dot(k_ref[here, c].T, ds, 1, 0)

    lax.fori_loop(0, iq, lambda j, _: block(j, False), None)
    block(iq, True)
    for h, c in enumerate(cut):
        dq = (dq_s[h] * scale).T.astype(LOW).astype(WIDE)
        dq_ref[:, c] = _turn(dq, cosq[...], -sinq[...]).astype(LOW)

    @pl.when(iq == pl.num_programs(1) - 1)
    def _():
        for c in cut:
            dk = (dk_s[:, c] * scale).astype(LOW).astype(WIDE)
            dk_ref[:, c] = _turn(dk, cosk[...], -sink[...]).astype(LOW)
            dv_ref[:, c] = dv_s[:, c].astype(LOW)


def attend_bwd(me, qkv, do, o, lse, cos, sin, slots, heads=3):
    total, wide = o.shape
    rows, parts = total // slots, wide // HEAD // heads
    width = heads * HEAD
    at = lambda g, i, me_ref: (_slot(i, me_ref[0], slots), g)
    queries = pl.BlockSpec((rows, width), at)
    keys = pl.BlockSpec((total, width), lambda g, i, me_ref: (0, g))
    within = lambda n: pl.BlockSpec((total, width), lambda g, i, me_ref: (0, n * parts + g))
    return pl.pallas_call(
        functools.partial(_backward, slots=slots),
        grid_spec=pltpu.PrefetchScalarGridSpec(
            num_scalar_prefetch=1,
            grid=(parts, slots),
            in_specs=[queries, within(1), within(2), queries, queries,
                      pl.BlockSpec((1, parts * heads, rows), lambda g, i, me_ref: (_slot(i, me_ref[0], slots), 0, 0))]
            + [pl.BlockSpec((rows, HEAD), lambda g, i, me_ref: (_slot(i, me_ref[0], slots), 0))] * 2 + [_full((total, HEAD))] * 2,
            out_specs=[queries, keys, keys],
            scratch_shapes=[pltpu.VMEM((heads, HEAD, rows), WIDE), pltpu.VMEM((total, width), WIDE), pltpu.VMEM((total, width), WIDE),
                            pltpu.VMEM((rows, rows), jnp.int32)],
        ),
        out_shape=[_like((total, wide))] * 3,
        compiler_params=_params(),
        cost_estimate=_cost(10 * total * total * wide, [o] * 8, total * total * wide // HEAD),
        name="attend_bwd",
    )(me, qkv, qkv, qkv, do, o, lse, cos, sin, cos, sin)


def _by_normed(*refs, adds):
    dq, dk, dv, wq, wk, wv = refs[:6]
    out = refs[-1]
    for at in range(0, out.shape[1], 256):
        c = slice(at, at + 256)
        t = _dot(dq[...], wq[c, :], 1, 1) + _dot(dk[...], wk[c, :], 1, 1) + _dot(dv[...], wv[c, :], 1, 1)
        for more in refs[6 : 6 + adds]:
            t += more[:, c].astype(WIDE)
        out[:, c] = t.astype(out.dtype)


def by_normed(slot, slots, dqkv, w, first, columns, adds=(), dtype=LOW, tile=512):
    rows, wide = dqkv[0].shape[0] // slots, dqkv[0].shape[1]
    base = first // tile
    return pl.pallas_call(
        functools.partial(_by_normed, adds=len(adds)),
        grid=(columns // tile,),
        in_specs=[pl.BlockSpec((rows, wide), lambda i: (slot, 0))] * 3 + [pl.BlockSpec((tile, wide), lambda i: (base + i, 0))] * 3
        + [pl.BlockSpec((rows, tile), lambda i: (0, i))] * len(adds),
        out_specs=pl.BlockSpec((rows, tile), lambda i: (0, i)),
        out_shape=_like((rows, columns), dtype),
        compiler_params=_params(),
        cost_estimate=_cost(2 * rows * columns * 3 * wide, [*w, *adds]),
        name=f"by_normed{slot}_{first}",
    )(*dqkv, *w, *adds)


def _finish(t, la, lb, ra, rb, x_ref, dy, gain, dx_o, dg_o):
    half = la.shape[1]
    x = x_ref[...].astype(WIDE)
    d = x.shape[1]
    dn = jnp.concatenate([t[:, :half] + la[...].astype(WIDE) + ra[...].astype(WIDE), t[:, half:] + lb[...].astype(WIDE) + rb[...].astype(WIDE)], 1)
    scale = lax.rsqrt(jnp.mean(x * x, -1, keepdims=True) + 1e-6)
    there = x * scale

    @pl.when(pl.program_id(0) == 0)
    def _():
        dg_o[...] = jnp.zeros_like(dg_o)

    dg_o[...] += (dn * there).reshape(-1, 8, d).sum(0)
    dh = dn * gain[...].astype(WIDE)
    dx = scale * (dh - there * jnp.mean(dh * there, -1, keepdims=True))
    dx_o[...] = (dx + dy[...].astype(WIDE)).astype(LOW)


def finish(t, la, lb, ra, rb, x, dy, gain, step=128):
    rows, d = x.shape
    full, half = pl.BlockSpec((step, d), lambda i: (i, 0)), pl.BlockSpec((step, d // 2), lambda i: (i, 0))
    return pl.pallas_call(
        _finish,
        grid=(rows // step,),
        in_specs=[full, half, half, half, half, full, full, _full(gain.shape)],
        out_specs=[full, _full((8, d))],
        out_shape=[_like((rows, d)), _like((8, d), WIDE)],
        compiler_params=_params(),
        cost_estimate=_cost(20 * rows * d, [t, x, x, x, x, x]),
        name="finish",
    )(t, la, lb, ra, rb, x, dy, gain)


def solution(mesh):
    slots = mesh.shape["tp"]
    right = [(i, (i + 1) % slots) for i in range(slots)]
    left = [(i, (i - 1) % slots) for i in range(slots)]

    def send(t, ring):
        return lax.ppermute(t, "tp", ring)

    def step(x, dy, gain, wq, wk, wv, wo):
        rows, d = x.shape
        total = slots * rows
        w = (wq, wk, wv)
        me = lax.axis_index("tp")
        me_s = me.astype(jnp.int32)[None]
        gain_row = gain[None]
        place = jnp.concatenate([lax.rem(me + s, slots) * rows + jnp.arange(rows) for s in range(slots)])
        half = HEAD // 2
        angle = place.astype(WIDE)[:, None] * THETA ** (-jnp.arange(half, dtype=WIDE) / half)
        c, s = jnp.cos(angle), jnp.sin(angle)
        cos, sin = jnp.concatenate([c, c], 1), jnp.concatenate([-s, s], 1)

        xs, dys, a, qkv, o, do, lse = front(x, dy, gain_row, cos, sin, wq, wk, wv, wo, slots)
        dqkv = attend_bwd(me_s, qkv, do, o, lse, cos, sin, slots)

        part = functools.partial(by_normed, slots=slots, w=w, columns=d // 2)
        term_a, term_b = part(2, dqkv=dqkv, first=0), part(2, dqkv=dqkv, first=d // 2)
        far_a, far_b = send(term_a, right), send(term_b, left)
        then, _ = lax.optimization_barrier((dqkv, (term_a, term_b)))
        term_b, term_a = part(1, dqkv=then, first=d // 2), part(3, dqkv=then, first=0)
        from_left_b, from_right_a = send(term_b, right), send(term_a, left)
        later, _ = lax.optimization_barrier((then, (term_a, term_b)))
        from_left_a = send(part(1, dqkv=then, first=0, adds=(far_a,)), right)
        from_right_b = send(part(3, dqkv=then, first=d // 2, adds=(far_b,)), left)
        own = by_normed(0, slots, later, w, 0, d, dtype=WIDE)
        dy_all = dys.reshape(total, d)
        by_w = [lax.dot_general(a, t, (((0,), (0,)), ((), ())), preferred_element_type=WIDE).astype(LOW) for t in later]
        by_wo = lax.dot_general(o, dy_all, (((0,), (0,)), ((), ())), preferred_element_type=WIDE).astype(LOW)
        by_x, by_gain = finish(own, from_left_a, from_left_b, from_right_a, from_right_b, x, dy, gain_row)
        by_gain = lax.psum(by_gain.sum(0)[None], "tp")
        return (by_x, by_gain, *by_w, by_wo)

    tokens, columns = P(("dp", "tp"), None), P(None, "tp")
    return jax.shard_map(
        step,
        mesh=mesh,
        in_specs=(tokens, tokens, P(None), columns, columns, columns, P("tp", None)),
        out_specs=(tokens, P("dp", None), P("dp", "tp"), P("dp", "tp"), P("dp", "tp"), P(("dp", "tp"), None)),
        check_vma=False,
    )
```

```python
import functools

import jax
import jax.numpy as jnp
from jax import lax
from jax.experimental import pallas as pl
from jax.experimental.pallas import tpu as pltpu
from jax.sharding import PartitionSpec as P

HEAD = 128
THETA = 10000
NEG = -1e30
HIDDEN = 2 * NEG
LOG2E = 1.4426950408889634
VMEM = 58 * 2**20
LOW = jnp.bfloat16
WIDE = jnp.float32


def _dot(a, b, ca, cb):
    return lax.dot_general(a, b, (((ca,), (cb,)), ((), ())), preferred_element_type=WIDE)


def _params(**more):
    return pltpu.CompilerParams(vmem_limit_bytes=VMEM, **more)


def _cost(flops, arrays, exps=0):
    return pl.CostEstimate(flops=int(flops), transcendentals=int(exps), bytes_accessed=int(sum(a.size * a.dtype.itemsize for a in arrays)))


def _like(shape, dtype=LOW):
    return jax.ShapeDtypeStruct(shape, dtype)


ANY = pl.BlockSpec(memory_space=pl.ANY)


def _full(shape):
    return pl.BlockSpec(shape, lambda *_: (0,) * len(shape))


def _turn(t, cos, sin):
    return t * cos + pltpu.roll(t, HEAD // 2, 1) * sin


def _slot(block, me, slots):
    return lax.rem(block - me + slots, slots)


def _gap(keys, queries):
    return lax.broadcasted_iota(jnp.int32, (keys, queries), 1) - lax.broadcasted_iota(jnp.int32, (keys, queries), 0)


def _front(x, dy, gain, cos, sin, wq, wk, wv, wo, xs, dys, a_o, d_o, o_o,
           wo_s, x_s, a_s, qkv_s, o_s, do_s, lse_s, gap_s, w_sem, x_sem, a_sem, out_sem, send_sem, recv_sem, *, slots, group):
    me = lax.axis_index("tp")
    rows, d = x.shape
    half, wide = rows // 2, wq.shape[1]
    heads = wide // HEAD
    right, left = lax.rem(me + 1, slots), lax.rem(me + slots - 1, slots)
    top, low = pl.ds(0, half), pl.ds(half, half)
    last = slots - 1
    scale = HEAD**-0.5
    e = scale * LOG2E

    barrier = pltpu.get_barrier_semaphore()
    for there in (left, right):
        pl.semaphore_signal(barrier, inc=1, device_id={"tp": there}, device_id_type=pl.DeviceIdType.MESH)
    pl.semaphore_wait(barrier, 2)

    def remote(n, src, dst, there):
        return pltpu.make_async_remote_copy(src_ref=src, dst_ref=dst, send_sem=send_sem.at[n], recv_sem=recv_sem.at[n],
                                            device_id={"tp": there}, device_id_type=pl.DeviceIdType.MESH)

    def transfers(n, t, ts):
        return [remote(n, t.at[top], ts.at[last, 0], right), remote(n + 1, t.at[low], ts.at[1, 1], left),
                remote(n + 2, t.at[low], ts.at[last, 1], right), remote(n + 3, t.at[top], ts.at[1, 0], left),
                remote(n + 4, ts.at[last, 0], ts.at[2, 0], right), remote(n + 5, ts.at[1, 1], ts.at[2, 1], left)]

    def start(copies):
        for copy in copies:
            copy.start()
        return copies

    def wait(copies):
        for copy in copies:
            copy.wait()

    def arrived(copies):
        for copy in copies:
            copy.wait_recv()

    x_go, dy_go = transfers(0, x, xs), transfers(6, dy, dys)
    start(x_go[:4])

    def into(ts, slot, p):
        return pltpu.make_async_copy(ts.at[slot, p], x_s.at[pl.ds(p * half, half)], x_sem.at[p])

    def own(t, p):
        return pltpu.make_async_copy(t.at[pl.ds(p * half, half)], x_s.at[pl.ds(p * half, half)], x_sem.at[p])

    def a_out(slot, p):
        return pltpu.make_async_copy(a_s.at[pl.ds(p * half, half)], a_o.at[pl.ds(slot * rows + p * half, half)], a_sem.at[p])

    loads = start([own(x, 0), own(x, 1)])
    wo_load = pltpu.make_async_copy(wo, wo_s, w_sem.at[3])
    gap_s[...] = _gap(rows, rows)
    g = gain[...].astype(WIDE)

    def by_seen(slot):
        at = slice(slot * rows, (slot + 1) * rows)

        def columns(i, _):
            c = pl.ds(pl.multiple_of(i * 256, 256), 256)
            do_s[at, c] = _dot(x_s[...], wo_s[c, :], 1, 1).astype(LOW)

        lax.fori_loop(0, wide // 256, columns, None)

    def head(n, h):
        return pl.ds(pl.multiple_of(n * wide + h * HEAD, HEAD), HEAD)

    def upward(w_s, top_s, mix_s):
        w_loads = start([pltpu.make_async_copy(w, w_s.at[:, pl.ds(i * wide, wide)], w_sem.at[i]) for i, w in enumerate((wq, wk, wv))])
        wo_load.start()
        top_s[...] = jnp.full_like(top_s, NEG)
        mix_s[...] = jnp.zeros_like(mix_s)

        def project(slot, p, before):
            if before is not None:
                a_out(*before).wait()
            for n in range(p * half, (p + 1) * half, 128):
                t = x_s[n : n + 128, :].astype(WIDE)
                size = lax.rsqrt(jnp.mean(t * t, -1, keepdims=True) + 1e-6)
                a_s[n : n + 128, :] = (t * size * g).astype(LOW)
            a_out(slot, p).start()
            if slot == 0 and p == 0:
                wait(w_loads)
            at, here = slice(slot * rows + p * half, slot * rows + (p + 1) * half), slice(p * half, (p + 1) * half)

            def turned(i, _):
                c = pl.ds(pl.multiple_of(i * 256, 256), 256)
                t = _dot(a_s[here, :], w_s[:, c], 1, 0).astype(LOW).astype(WIDE)
                qkv_s[at, c] = jnp.concatenate([_turn(t[:, h : h + HEAD], cos[at, :], sin[at, :]) for h in (0, HEAD)], 1).astype(LOW)

            def plain(i, _):
                c = pl.ds(pl.multiple_of(i * 256, 256), 256)
                qkv_s[at, c] = _dot(a_s[here, :], w_s[:, c], 1, 0).astype(LOW)

            lax.fori_loop(0, 2 * wide // 256, turned, None)
            lax.fori_loop(2 * wide // 256, 3 * wide // 256, plain, None)

        def pair(sq, sk, masked):
            mine, here = pl.ds(sq * rows, rows), pl.ds(sk * rows, rows)
            ones = jnp.ones((8, rows), LOW)
            scores = [_dot(qkv_s[here, head(1, h)], qkv_s[mine, head(0, h)], 1, 1) for h in range(heads)]
            weights, keeps = [], []
            for h, s in enumerate(scores):
                if masked:
                    s = jnp.where(gap_s[...] >= 0, s, HIDDEN)
                old = top_s[sq, h : h + 1, :]
                most = jnp.maximum(old, s.max(axis=0, keepdims=True))
                top_s[sq, h : h + 1, :] = most
                weights.append(jnp.exp2((s - most) * e).astype(LOW))
                keeps.append(jnp.exp2((old - most) * e))
            for h, (p, keep) in enumerate(zip(weights, keeps)):
                values = jnp.concatenate([qkv_s[here, head(2, h)].T, ones], axis=0)
                mix_s[sq, h] = mix_s[sq, h] * keep + _dot(values, p, 1, 0)

        wait(loads)
        project(0, 0, None)
        project(0, 1, None)
        wait(start([own(dy, 0), own(dy, 1)]))
        keep = start([pltpu.make_async_copy(x_s.at[pl.ds(p * half, half)], dys.at[0, p], x_sem.at[p]) for p in range(2)])
        wo_load.wait()
        by_seen(0)
        wait(keep)
        arrived(x_go[:2])
        start(x_go[4:])
        wait(start([into(xs, last, 0), into(xs, 1, 1)]))
        project(last, 0, (0, 0))
        project(1, 1, (0, 1))
        arrived(x_go[2:4])
        start(dy_go[:4])
        wait(start([into(xs, 1, 0), into(xs, last, 1)]))
        project(1, 0, (last, 0))
        project(last, 1, (1, 1))

        def step(n, _):
            @pl.when(n == 9)
            def _():
                arrived(x_go[4:])
                wait(start([into(xs, 2, 0), into(xs, 2, 1)]))
                project(2, 0, (1, 0))
                project(2, 1, (last, 1))

            i, j = n // 3, n % 3
            m = n - 9
            sq = jnp.where(n < 9, i + i // 2, jnp.where(m < 4, 2, m - 4 + (m - 4) // 2))
            sk = jnp.where(n < 9, j + j // 2, jnp.where(m < 4, m, 2))
            bq, bk = lax.rem(me + sq, slots), lax.rem(me + sk, slots)

            @pl.when(bk < bq)
            def _():
                pair(sq, sk, False)

            @pl.when(bk == bq)
            def _():
                pair(sq, sk, True)

        lax.fori_loop(0, slots * slots, step, None)
        for slot in range(slots):
            for h in range(heads):
                total = mix_s[slot, h, HEAD : HEAD + 1, :]
                o_s[slot * rows : (slot + 1) * rows, head(0, h)] = (mix_s[slot, h, :HEAD, :] * (1 / total)).T.astype(LOW)
                lse_s[slot, h : h + 1, :] = top_s[slot, h : h + 1, :] * e + jnp.log2(total)
        wait([a_out(2, 0), a_out(2, 1)])

    pl.run_scoped(upward, pltpu.VMEM((d, 3 * wide), LOW), pltpu.VMEM((slots, heads, rows), WIDE),
                  pltpu.VMEM((slots, heads, HEAD + 8, rows), WIDE))
    o_out = start([pltpu.make_async_copy(o_s, o_o, w_sem.at[0])])
    arrived(dy_go[:2])
    start(dy_go[4:])

    def d_out(slot):
        at = pl.ds(slot * rows, rows)
        return pltpu.make_async_copy(qkv_s.at[at], d_o.at[at], out_sem.at[slot])

    def downward(dq_s, dk_s, dv_s):
        dk_s[...] = jnp.zeros_like(dk_s)
        dv_s[...] = jnp.zeros_like(dv_s)

        def step(n, _):
            @pl.when(n == 1)
            def _():
                arrived(dy_go[2:4])
                for slot in (1, last):
                    wait(start([into(dys, slot, 0), into(dys, slot, 1)]))
                    by_seen(slot)

            @pl.when(n == 3)
            def _():
                arrived(dy_go[4:])
                wait(start([into(dys, 2, 0), into(dys, 2, 1)]))
                by_seen(2)

            sq = jnp.where(n < 2, n, 5 - n)
            bq = lax.rem(me + sq, slots)
            mine = pl.ds(sq * rows, rows)

            def some(k, _):
                hs = [k * group + h for h in range(group)]
                cut = [head(0, h) for h in hs]
                dq_s[...] = jnp.zeros_like(dq_s)
                lses = [lse_s[sq, pl.ds(h, 1), :] for h in hs]
                deltas = [(do_s[mine, c].astype(WIDE) * o_s[mine, c].astype(WIDE)).T.sum(axis=0, keepdims=True) for c in cut]

                def block(j, masked):
                    here = pl.ds(_slot(j, me, slots) * rows, rows)
                    scores = [_dot(qkv_s[here, head(1, h)], qkv_s[mine, head(0, h)], 1, 1) for h in hs]
                    dps = [_dot(qkv_s[here, head(2, h)], do_s[mine, c], 1, 1) for h, c in zip(hs, cut)]
                    for i, (h, c) in enumerate(zip(hs, cut)):
                        p = jnp.exp2(scores[i] * e - lses[i])
                        if masked:
                            p = jnp.where(gap_s[...] >= 0, p, 0.0)
                        ds = (p * (dps[i] - deltas[i])).astype(LOW)
                        dv_s[here, c] += _dot(p.astype(LOW), do_s[mine, c], 1, 0)
                        dk_s[here, c] += _dot(ds, qkv_s[mine, c], 1, 0)
                        dq_s[i] += _dot(qkv_s[here, head(1, h)].T, ds, 1, 0)

                lax.fori_loop(0, bq, lambda j, _: block(j, False), None)
                block(bq, True)
                for i, c in enumerate(cut):
                    dq = (dq_s[i] * scale).T.astype(LOW).astype(WIDE)
                    qkv_s[mine, c] = _turn(dq, cos[mine, :], -sin[mine, :]).astype(LOW)

            lax.fori_loop(0, heads // group, some, None)

        lax.fori_loop(0, slots, step, None)

        def finish(slot, _):
            at = pl.ds(slot * rows, rows)
            for h in range(heads):
                c = head(0, h)
                dk = (dk_s[at, c] * scale).astype(LOW).astype(WIDE)
                qkv_s[at, head(1, h)] = _turn(dk, cos[at, :], -sin[at, :]).astype(LOW)
                qkv_s[at, head(2, h)] = dv_s[at, c].astype(LOW)
            d_out(slot).start()

        lax.fori_loop(0, slots, finish, None)

    pl.run_scoped(downward, pltpu.VMEM((group, HEAD, rows), WIDE), pltpu.VMEM((slots * rows, wide), WIDE),
                  pltpu.VMEM((slots * rows, wide), WIDE))
    wait(o_out)
    wait([d_out(slot) for slot in range(slots)])
    for copy in (*x_go, *dy_go):
        copy.wait_send()


def front(x, dy, gain, cos, sin, wq, wk, wv, wo, slots, group=3):
    rows, d = x.shape
    wide = wq.shape[1]
    total, heads = slots * rows, wide // HEAD
    blocks = _like((slots, 2, rows // 2, d))
    copies = pltpu.SemaphoreType.DMA((12,))
    return pl.pallas_call(
        functools.partial(_front, slots=slots, group=group),
        in_specs=[ANY, ANY] + [pl.BlockSpec(memory_space=pltpu.VMEM)] * 3 + [ANY] * 4,
        out_specs=[ANY] * 5,
        out_shape=[blocks, blocks, _like((total, d)), _like((total, 3 * wide)), _like((total, wide))],
        scratch_shapes=[pltpu.VMEM((wide, d), LOW), pltpu.VMEM((rows, d), LOW), pltpu.VMEM((rows, d), LOW),
                        pltpu.VMEM((total, 3 * wide), LOW), pltpu.VMEM((total, wide), LOW), pltpu.VMEM((total, wide), LOW),
                        pltpu.VMEM((slots, heads, rows), WIDE), pltpu.VMEM((rows, rows), jnp.int32),
                        pltpu.SemaphoreType.DMA((4,)), pltpu.SemaphoreType.DMA((2,)), pltpu.SemaphoreType.DMA((2,)),
                        pltpu.SemaphoreType.DMA((slots,)), copies, copies],
        compiler_params=_params(collective_id=0, has_side_effects=True),
        cost_estimate=_cost(2 * total * d * 4 * wide + 14 * total * total * wide, [x] * 20, 2 * total * total * heads),
        name="front",
    )(x, dy, gain, cos, sin, wq, wk, wv, wo)


def _by_normed(*refs, adds):
    dq, dk, dv, wq, wk, wv = refs[:6]
    out = refs[-1]
    for at in range(0, out.shape[1], 256):
        c = slice(at, at + 256)
        t = _dot(dq[...], wq[c, :], 1, 1) + _dot(dk[...], wk[c, :], 1, 1) + _dot(dv[...], wv[c, :], 1, 1)
        for more in refs[6 : 6 + adds]:
            t += more[:, c].astype(WIDE)
        out[:, c] = t.astype(out.dtype)


def by_normed(slot, slots, dqkv, w, first, columns, adds=(), dtype=LOW, tile=512):
    rows, wide = dqkv.shape[0] // slots, w[0].shape[1]
    base = first // tile
    return pl.pallas_call(
        functools.partial(_by_normed, adds=len(adds)),
        grid=(columns // tile,),
        in_specs=[pl.BlockSpec((rows, wide), lambda i, n=n: (slot, n)) for n in range(3)] + [pl.BlockSpec((tile, wide), lambda i: (base + i, 0))] * 3
        + [pl.BlockSpec((rows, tile), lambda i: (0, i))] * len(adds),
        out_specs=pl.BlockSpec((rows, tile), lambda i: (0, i)),
        out_shape=_like((rows, columns), dtype),
        compiler_params=_params(),
        cost_estimate=_cost(2 * rows * columns * 3 * wide, [*w, *adds]),
        name=f"by_normed{slot}_{first}",
    )(dqkv, dqkv, dqkv, *w, *adds)


def _finish(t, la, lb, ra, rb, x_ref, dy, gain, dx_o, dg_o):
    half = la.shape[1]
    x = x_ref[...].astype(WIDE)
    d = x.shape[1]
    dn = jnp.concatenate([t[:, :half] + la[...].astype(WIDE) + ra[...].astype(WIDE), t[:, half:] + lb[...].astype(WIDE) + rb[...].astype(WIDE)], 1)
    scale = lax.rsqrt(jnp.mean(x * x, -1, keepdims=True) + 1e-6)
    there = x * scale

    @pl.when(pl.program_id(0) == 0)
    def _():
        dg_o[...] = jnp.zeros_like(dg_o)

    dg_o[...] += (dn * there).reshape(-1, 8, d).sum(0)
    dh = dn * gain[...].astype(WIDE)
    dx = scale * (dh - there * jnp.mean(dh * there, -1, keepdims=True))
    dx_o[...] = (dx + dy[...].astype(WIDE)).astype(LOW)


def finish(t, la, lb, ra, rb, x, dy, gain, step=128):
    rows, d = x.shape
    full, half = pl.BlockSpec((step, d), lambda i: (i, 0)), pl.BlockSpec((step, d // 2), lambda i: (i, 0))
    return pl.pallas_call(
        _finish,
        grid=(rows // step,),
        in_specs=[full, half, half, half, half, full, full, _full(gain.shape)],
        out_specs=[full, _full((8, d))],
        out_shape=[_like((rows, d)), _like((8, d), WIDE)],
        compiler_params=_params(),
        cost_estimate=_cost(20 * rows * d, [t, x, x, x, x, x]),
        name="finish",
    )(t, la, lb, ra, rb, x, dy, gain)


def solution(mesh):
    slots = mesh.shape["tp"]
    right = [(i, (i + 1) % slots) for i in range(slots)]
    left = [(i, (i - 1) % slots) for i in range(slots)]

    def send(t, ring):
        return lax.ppermute(t, "tp", ring)

    def step(x, dy, gain, wq, wk, wv, wo):
        rows, d = x.shape
        total = slots * rows
        w = (wq, wk, wv)
        me = lax.axis_index("tp")
        gain_row = gain[None]
        place = jnp.concatenate([lax.rem(me + s, slots) * rows + jnp.arange(rows) for s in range(slots)])
        half = HEAD // 2
        angle = place.astype(WIDE)[:, None] * THETA ** (-jnp.arange(half, dtype=WIDE) / half)
        c, s = jnp.cos(angle), jnp.sin(angle)
        cos, sin = jnp.concatenate([c, c], 1), jnp.concatenate([-s, s], 1)

        _, dys, a, dqkv, o = front(x, dy, gain_row, cos, sin, wq, wk, wv, wo, slots)

        part = functools.partial(by_normed, slots=slots, w=w, columns=d // 2)
        term_a, term_b = part(2, dqkv=dqkv, first=0), part(2, dqkv=dqkv, first=d // 2)
        far_a, far_b = send(term_a, right), send(term_b, left)
        then, _ = lax.optimization_barrier((dqkv, (term_a, term_b)))
        term_b, term_a = part(1, dqkv=then, first=d // 2), part(3, dqkv=then, first=0)
        from_left_b, from_right_a = send(term_b, right), send(term_a, left)
        later, _ = lax.optimization_barrier((then, (term_a, term_b)))
        from_left_a = send(part(1, dqkv=then, first=0, adds=(far_a,)), right)
        from_right_b = send(part(3, dqkv=then, first=d // 2, adds=(far_b,)), left)
        own = by_normed(0, slots, later, w, 0, d, dtype=WIDE)
        dy_all = dys.reshape(total, d)
        by_w = [lax.dot_general(a, t, (((0,), (0,)), ((), ())), preferred_element_type=WIDE).astype(LOW) for t in jnp.split(later, 3, 1)]
        by_wo = lax.dot_general(o, dy_all, (((0,), (0,)), ((), ())), preferred_element_type=WIDE).astype(LOW)
        by_x, by_gain = finish(own, from_left_a, from_left_b, from_right_a, from_right_b, x, dy, gain_row)
        by_gain = lax.psum(by_gain.sum(0)[None], "tp")
        return (by_x, by_gain, *by_w, by_wo)

    tokens, columns = P(("dp", "tp"), None), P(None, "tp")
    return jax.shard_map(
        step,
        mesh=mesh,
        in_specs=(tokens, tokens, P(None), columns, columns, columns, P("tp", None)),
        out_specs=(tokens, P("dp", None), P("dp", "tp"), P("dp", "tp"), P("dp", "tp"), P(("dp", "tp"), None)),
        check_vma=False,
    )
```

```python
import functools

import jax
import jax.numpy as jnp
from jax import lax
from jax.experimental import pallas as pl
from jax.experimental.pallas import tpu as pltpu
from jax.sharding import PartitionSpec as P

HEAD = 128
THETA = 10000
NEG = -1e30
HIDDEN = 2 * NEG
LOG2E = 1.4426950408889634
VMEM = 58 * 2**20
LOW = jnp.bfloat16
WIDE = jnp.float32


def _dot(a, b, ca, cb):
    return lax.dot_general(a, b, (((ca,), (cb,)), ((), ())), preferred_element_type=WIDE)


def _params(**more):
    return pltpu.CompilerParams(vmem_limit_bytes=VMEM, **more)


def _cost(flops, arrays, exps=0):
    return pl.CostEstimate(flops=int(flops), transcendentals=int(exps), bytes_accessed=int(sum(a.size * a.dtype.itemsize for a in arrays)))


def _like(shape, dtype=LOW):
    return jax.ShapeDtypeStruct(shape, dtype)


ANY = pl.BlockSpec(memory_space=pl.ANY)


def _full(shape):
    return pl.BlockSpec(shape, lambda *_: (0,) * len(shape))


def _turn(t, cos, sin):
    return t * cos + pltpu.roll(t, HEAD // 2, 1) * sin


def _slot(block, me, slots):
    return lax.rem(block - me + slots, slots)


def _gap(keys, queries):
    return lax.broadcasted_iota(jnp.int32, (keys, queries), 1) - lax.broadcasted_iota(jnp.int32, (keys, queries), 0)


def _front(x, dy, gain, pace, wq, wk, wv, wo, xs, dys, a_o, d_o, o_o,
           wo_s, x_s, a_s, qkv_s, o_s, do_s, lse_s, gap_s, cos, sin, w_sem, x_sem, a_sem, out_sem, send_sem, recv_sem, *, slots, group):
    me = lax.axis_index("tp")
    rows, d = x.shape
    half, wide = rows // 2, wq.shape[1]
    heads = wide // HEAD
    right, left = lax.rem(me + 1, slots), lax.rem(me + slots - 1, slots)
    top, low = pl.ds(0, half), pl.ds(half, half)
    last = slots - 1
    scale = HEAD**-0.5
    e = scale * LOG2E

    barrier = pltpu.get_barrier_semaphore()
    for there in (left, right):
        pl.semaphore_signal(barrier, inc=1, device_id={"tp": there}, device_id_type=pl.DeviceIdType.MESH)
    pl.semaphore_wait(barrier, 2)

    def remote(n, src, dst, there):
        return pltpu.make_async_remote_copy(src_ref=src, dst_ref=dst, send_sem=send_sem.at[n], recv_sem=recv_sem.at[n],
                                            device_id={"tp": there}, device_id_type=pl.DeviceIdType.MESH)

    def transfers(n, t, ts):
        return [remote(n, t.at[top], ts.at[last, 0], right), remote(n + 1, t.at[low], ts.at[1, 1], left),
                remote(n + 2, t.at[low], ts.at[last, 1], right), remote(n + 3, t.at[top], ts.at[1, 0], left),
                remote(n + 4, ts.at[last, 0], ts.at[2, 0], right), remote(n + 5, ts.at[1, 1], ts.at[2, 1], left)]

    def start(copies):
        for copy in copies:
            copy.start()
        return copies

    def wait(copies):
        for copy in copies:
            copy.wait()

    def arrived(copies):
        for copy in copies:
            copy.wait_recv()

    x_go, dy_go = transfers(0, x, xs), transfers(6, dy, dys)
    start(x_go[:4])

    def into(ts, slot, p):
        return pltpu.make_async_copy(ts.at[slot, p], x_s.at[pl.ds(p * half, half)], x_sem.at[p])

    def own(t, p):
        return pltpu.make_async_copy(t.at[pl.ds(p * half, half)], x_s.at[pl.ds(p * half, half)], x_sem.at[p])

    def a_out(slot, p):
        return pltpu.make_async_copy(a_s.at[pl.ds(p * half, half)], a_o.at[pl.ds(slot * rows + p * half, half)], a_sem.at[p])

    loads = start([own(x, 0), own(x, 1)])
    wo_load = pltpu.make_async_copy(wo, wo_s, w_sem.at[3])
    gap_s[...] = _gap(rows, rows)

    def table(n, _):
        at = pl.ds(pl.multiple_of(n * 128, 128), 128)
        first = lax.rem(me + n * 128 // rows, slots) * rows + lax.rem(n * 128, rows)
        angle = (first + lax.broadcasted_iota(jnp.int32, (128, HEAD), 0)).astype(WIDE) * pace[...]
        cos[at, :] = jnp.cos(angle)
        sin[at, :] = jnp.where(lax.broadcasted_iota(jnp.int32, (128, HEAD), 1) < HEAD // 2, -1.0, 1.0) * jnp.sin(angle)

    lax.fori_loop(0, slots * rows // 128, table, None)
    g = gain[...].astype(WIDE)

    def by_seen(slot):
        at = slice(slot * rows, (slot + 1) * rows)

        def columns(i, _):
            c = pl.ds(pl.multiple_of(i * 256, 256), 256)
            do_s[at, c] = _dot(x_s[...], wo_s[c, :], 1, 1).astype(LOW)

        lax.fori_loop(0, wide // 256, columns, None)

    def head(n, h):
        return pl.ds(pl.multiple_of(n * wide + h * HEAD, HEAD), HEAD)

    def upward(w_s, top_s, mix_s):
        w_loads = start([pltpu.make_async_copy(w, w_s.at[:, pl.ds(i * wide, wide)], w_sem.at[i]) for i, w in enumerate((wq, wk, wv))])
        wo_load.start()
        top_s[...] = jnp.full_like(top_s, NEG)
        mix_s[...] = jnp.zeros_like(mix_s)

        def project(slot, p, before):
            if before is not None:
                a_out(*before).wait()
            for n in range(p * half, (p + 1) * half, 128):
                t = x_s[n : n + 128, :].astype(WIDE)
                size = lax.rsqrt(jnp.mean(t * t, -1, keepdims=True) + 1e-6)
                a_s[n : n + 128, :] = (t * size * g).astype(LOW)
            a_out(slot, p).start()
            if slot == 0 and p == 0:
                wait(w_loads)
            at, here = slice(slot * rows + p * half, slot * rows + (p + 1) * half), slice(p * half, (p + 1) * half)

            def turned(i, _):
                c = pl.ds(pl.multiple_of(i * 256, 256), 256)
                t = _dot(a_s[here, :], w_s[:, c], 1, 0).astype(LOW).astype(WIDE)
                qkv_s[at, c] = jnp.concatenate([_turn(t[:, h : h + HEAD], cos[at, :], sin[at, :]) for h in (0, HEAD)], 1).astype(LOW)

            def plain(i, _):
                c = pl.ds(pl.multiple_of(i * 256, 256), 256)
                qkv_s[at, c] = _dot(a_s[here, :], w_s[:, c], 1, 0).astype(LOW)

            lax.fori_loop(0, 2 * wide // 256, turned, None)
            lax.fori_loop(2 * wide // 256, 3 * wide // 256, plain, None)

        def pair(sq, sk, masked):
            mine, here = pl.ds(sq * rows, rows), pl.ds(sk * rows, rows)
            ones = jnp.ones((8, rows), LOW)
            scores = [_dot(qkv_s[here, head(1, h)], qkv_s[mine, head(0, h)], 1, 1) for h in range(heads)]
            weights, keeps = [], []
            for h, s in enumerate(scores):
                if masked:
                    s = jnp.where(gap_s[...] >= 0, s, HIDDEN)
                old = top_s[sq, h : h + 1, :]
                most = jnp.maximum(old, s.max(axis=0, keepdims=True))
                top_s[sq, h : h + 1, :] = most
                weights.append(jnp.exp2((s - most) * e).astype(LOW))
                keeps.append(jnp.exp2((old - most) * e))
            for h, (p, keep) in enumerate(zip(weights, keeps)):
                values = jnp.concatenate([qkv_s[here, head(2, h)].T, ones], axis=0)
                mix_s[sq, h] = mix_s[sq, h] * keep + _dot(values, p, 1, 0)

        wait(loads)
        project(0, 0, None)
        project(0, 1, None)
        wait(start([own(dy, 0), own(dy, 1)]))
        keep = start([pltpu.make_async_copy(x_s.at[pl.ds(p * half, half)], dys.at[0, p], x_sem.at[p]) for p in range(2)])
        wo_load.wait()
        by_seen(0)
        wait(keep)
        arrived(x_go[:2])
        start(x_go[4:])
        wait(start([into(xs, last, 0), into(xs, 1, 1)]))
        project(last, 0, (0, 0))
        project(1, 1, (0, 1))
        arrived(x_go[2:4])
        start(dy_go[:4])
        wait(start([into(xs, 1, 0), into(xs, last, 1)]))
        project(1, 0, (last, 0))
        project(last, 1, (1, 1))

        def step(n, _):
            @pl.when(n == 9)
            def _():
                arrived(x_go[4:])
                wait(start([into(xs, 2, 0), into(xs, 2, 1)]))
                project(2, 0, (1, 0))
                project(2, 1, (last, 1))

            i, j = n // 3, n % 3
            m = n - 9
            sq = jnp.where(n < 9, i + i // 2, jnp.where(m < 4, 2, m - 4 + (m - 4) // 2))
            sk = jnp.where(n < 9, j + j // 2, jnp.where(m < 4, m, 2))
            bq, bk = lax.rem(me + sq, slots), lax.rem(me + sk, slots)

            @pl.when(bk < bq)
            def _():
                pair(sq, sk, False)

            @pl.when(bk == bq)
            def _():
                pair(sq, sk, True)

        lax.fori_loop(0, slots * slots, step, None)
        for slot in range(slots):
            for h in range(heads):
                total = mix_s[slot, h, HEAD : HEAD + 1, :]
                o_s[slot * rows : (slot + 1) * rows, head(0, h)] = (mix_s[slot, h, :HEAD, :] * (1 / total)).T.astype(LOW)
                lse_s[slot, h : h + 1, :] = top_s[slot, h : h + 1, :] * e + jnp.log2(total)
        wait([a_out(2, 0), a_out(2, 1)])

    pl.run_scoped(upward, pltpu.VMEM((d, 3 * wide), LOW), pltpu.VMEM((slots, heads, rows), WIDE),
                  pltpu.VMEM((slots, heads, HEAD + 8, rows), WIDE))
    o_out = start([pltpu.make_async_copy(o_s, o_o, w_sem.at[0])])
    arrived(dy_go[:2])
    start(dy_go[4:])

    def d_out(slot):
        at = pl.ds(slot * rows, rows)
        return pltpu.make_async_copy(qkv_s.at[at], d_o.at[at], out_sem.at[slot])

    def downward(dq_s, dk_s, dv_s):
        dk_s[...] = jnp.zeros_like(dk_s)
        dv_s[...] = jnp.zeros_like(dv_s)

        def step(n, _):
            @pl.when(n == 1)
            def _():
                arrived(dy_go[2:4])
                for slot in (1, last):
                    wait(start([into(dys, slot, 0), into(dys, slot, 1)]))
                    by_seen(slot)

            @pl.when(n == 3)
            def _():
                arrived(dy_go[4:])
                wait(start([into(dys, 2, 0), into(dys, 2, 1)]))
                by_seen(2)

            sq = jnp.where(n < 2, n, 5 - n)
            bq = lax.rem(me + sq, slots)
            mine = pl.ds(sq * rows, rows)

            def some(k, _):
                hs = [k * group + h for h in range(group)]
                cut = [head(0, h) for h in hs]
                dq_s[...] = jnp.zeros_like(dq_s)
                lses = [lse_s[sq, pl.ds(h, 1), :] for h in hs]
                deltas = [(do_s[mine, c].astype(WIDE) * o_s[mine, c].astype(WIDE)).T.sum(axis=0, keepdims=True) for c in cut]

                def block(j, masked):
                    here = pl.ds(_slot(j, me, slots) * rows, rows)
                    scores = [_dot(qkv_s[here, head(1, h)], qkv_s[mine, head(0, h)], 1, 1) for h in hs]
                    dps = [_dot(qkv_s[here, head(2, h)], do_s[mine, c], 1, 1) for h, c in zip(hs, cut)]
                    for i, (h, c) in enumerate(zip(hs, cut)):
                        p = jnp.exp2(scores[i] * e - lses[i])
                        if masked:
                            p = jnp.where(gap_s[...] >= 0, p, 0.0)
                        ds = (p * (dps[i] - deltas[i])).astype(LOW)
                        dv_s[here, c] += _dot(p.astype(LOW), do_s[mine, c], 1, 0)
                        dk_s[here, c] += _dot(ds, qkv_s[mine, c], 1, 0)
                        dq_s[i] += _dot(qkv_s[here, head(1, h)].T, ds, 1, 0)

                lax.fori_loop(0, bq, lambda j, _: block(j, False), None)
                block(bq, True)
                for i, c in enumerate(cut):
                    dq = (dq_s[i] * scale).T.astype(LOW).astype(WIDE)
                    qkv_s[mine, c] = _turn(dq, cos[mine, :], -sin[mine, :]).astype(LOW)

            lax.fori_loop(0, heads // group, some, None)

        lax.fori_loop(0, slots, step, None)

        def finish(slot, _):
            at = pl.ds(slot * rows, rows)
            for h in range(heads):
                c = head(0, h)
                dk = (dk_s[at, c] * scale).astype(LOW).astype(WIDE)
                qkv_s[at, head(1, h)] = _turn(dk, cos[at, :], -sin[at, :]).astype(LOW)
                qkv_s[at, head(2, h)] = dv_s[at, c].astype(LOW)
            d_out(slot).start()

        lax.fori_loop(0, slots, finish, None)

    pl.run_scoped(downward, pltpu.VMEM((group, HEAD, rows), WIDE), pltpu.VMEM((slots * rows, wide), WIDE),
                  pltpu.VMEM((slots * rows, wide), WIDE))
    wait(o_out)
    wait([d_out(slot) for slot in range(slots)])
    for copy in (*x_go, *dy_go):
        copy.wait_send()


def front(x, dy, gain, pace, wq, wk, wv, wo, slots, group=3):
    rows, d = x.shape
    wide = wq.shape[1]
    total, heads = slots * rows, wide // HEAD
    blocks = _like((slots, 2, rows // 2, d))
    copies = pltpu.SemaphoreType.DMA((12,))
    return pl.pallas_call(
        functools.partial(_front, slots=slots, group=group),
        in_specs=[ANY, ANY] + [pl.BlockSpec(memory_space=pltpu.VMEM)] * 2 + [ANY] * 4,
        out_specs=[ANY] * 5,
        out_shape=[blocks, blocks, _like((total, d)), _like((total, 3 * wide)), _like((total, wide))],
        scratch_shapes=[pltpu.VMEM((wide, d), LOW), pltpu.VMEM((rows, d), LOW), pltpu.VMEM((rows, d), LOW),
                        pltpu.VMEM((total, 3 * wide), LOW), pltpu.VMEM((total, wide), LOW), pltpu.VMEM((total, wide), LOW),
                        pltpu.VMEM((slots, heads, rows), WIDE), pltpu.VMEM((rows, rows), jnp.int32),
                        pltpu.VMEM((total, HEAD), WIDE), pltpu.VMEM((total, HEAD), WIDE), pltpu.SemaphoreType.DMA((4,)), pltpu.SemaphoreType.DMA((2,)), pltpu.SemaphoreType.DMA((2,)),
                        pltpu.SemaphoreType.DMA((slots,)), copies, copies],
        compiler_params=_params(collective_id=0, has_side_effects=True),
        cost_estimate=_cost(2 * total * d * 4 * wide + 14 * total * total * wide, [x] * 20, 2 * total * total * heads),
        name="front",
    )(x, dy, gain, pace, wq, wk, wv, wo)


def _terms(d_i, wq, wk, wv, right_o, left_o, own_o, d_s, w_s, far_s, got_s, wide_s, low_s, own_s, w_sem, d_sem, out_sem, send_sem, recv_sem, *, slots):
    me = lax.axis_index("tp")
    rows, d = own_o.shape
    wide = wq.shape[1]
    right, left = lax.rem(me + 1, slots), lax.rem(me + slots - 1, slots)
    last, half, tile = slots - 1, d // 2, 256
    tiles = d // tile

    def d_in(slot):
        return pltpu.make_async_copy(d_i.at[pl.ds(slot * rows, rows)], d_s.at[slot], d_sem.at[slot])

    def w_in(i, n):
        return pltpu.make_async_copy((wq, wk, wv)[i].at[pl.ds(n * tile, tile)], w_s.at[pl.ds(n * tile, tile), pl.ds(i * wide, wide)], w_sem.at[i, n])

    d_in(2).start()
    for n in range(tiles):
        for i in range(3):
            w_in(i, n).start()
    for slot in (1, last, 0):
        d_in(slot).start()
    barrier = pltpu.get_barrier_semaphore()
    for there in (left, right):
        pl.semaphore_signal(barrier, inc=1, device_id={"tp": there}, device_id_type=pl.DeviceIdType.MESH)
    pl.semaphore_wait(barrier, 2)
    sends = [pltpu.make_async_remote_copy(src_ref=far_s.at[p], dst_ref=got_s.at[p], send_sem=send_sem.at[p], recv_sem=recv_sem.at[p],
                                          device_id={"tp": there}, device_id_type=pl.DeviceIdType.MESH) for p, there in enumerate((right, left))]

    def columns(n):
        return pl.ds(pl.multiple_of(n * tile, tile), tile)

    def term(slot, n):
        return _dot(d_s[slot], w_s[columns(n), :], 1, 1)

    d_in(2).wait()

    def far(n, _):
        for i in range(3):
            w_in(i, n).wait()
        far_s[n // (tiles // 2), :, columns(n % (tiles // 2))] = term(2, n).astype(LOW)

        @pl.when(n == tiles // 2)
        def _():
            sends[0].start()

    lax.fori_loop(0, tiles, far, None)
    for slot in (1, last, 0):
        d_in(slot).wait()

    def near(n, _):
        m = n + tiles // 2
        low_s[0, :, columns(m)] = term(1, m).astype(LOW)

        @pl.when(n == 0)
        def _():
            sends[1].start()

        low_s[1, :, columns(n)] = term(last, n).astype(LOW)
        wide_s[0, :, columns(n)] = term(1, n)
        wide_s[1, :, columns(n)] = term(last, m)

    lax.fori_loop(0, tiles // 2, near, None)

    def own(n, _):
        own_s[:, columns(n)] = term(0, n)

    lax.fori_loop(0, tiles, own, None)
    own_out = pltpu.make_async_copy(own_s, own_o, out_sem.at[2])
    own_out.start()
    sends[0].wait_recv()
    sends[1].wait_recv()

    def add(n, _):
        at = pl.ds(pl.multiple_of(n * 64, 64), 64)
        low_s[0, at, :half] = (wide_s[0, at, :] + got_s[0, at, :].astype(WIDE)).astype(LOW)
        low_s[1, at, half:] = (wide_s[1, at, :] + got_s[1, at, :].astype(WIDE)).astype(LOW)

    lax.fori_loop(0, rows // 64, add, None)
    outs = [pltpu.make_async_copy(low_s.at[p], o, out_sem.at[p]) for p, o in enumerate((right_o, left_o))]
    for copy in outs:
        copy.start()
    for copy in (*outs, own_out):
        copy.wait()
    for copy in sends:
        copy.wait_send()


def terms(dqkv, wq, wk, wv, slots):
    d, wide = wq.shape
    rows = dqkv.shape[0] // slots
    two = pltpu.SemaphoreType.DMA((2,))
    return pl.pallas_call(
        functools.partial(_terms, slots=slots),
        in_specs=[ANY] * 4,
        out_specs=[ANY] * 3,
        out_shape=[_like((rows, d)), _like((rows, d)), _like((rows, d), WIDE)],
        scratch_shapes=[pltpu.VMEM((slots, rows, 3 * wide), LOW), pltpu.VMEM((d, 3 * wide), LOW), pltpu.VMEM((2, rows, d // 2), LOW),
                        pltpu.VMEM((2, rows, d // 2), LOW), pltpu.VMEM((2, rows, d // 2), WIDE), pltpu.VMEM((2, rows, d), LOW),
                        pltpu.VMEM((rows, d), WIDE), pltpu.SemaphoreType.DMA((3, d // 256)), pltpu.SemaphoreType.DMA((slots,)),
                        pltpu.SemaphoreType.DMA((3,)), two, two],
        compiler_params=_params(collective_id=1, has_side_effects=True),
        cost_estimate=_cost(6 * slots * rows * d * wide, [dqkv, wq, wk, wv]),
        name="terms",
    )(dqkv, wq, wk, wv)


def _finish(own, from_left, from_right, x_ref, dy, gain, dx_o, dg_o, dg_s):
    x = x_ref[...].astype(WIDE)
    d = x.shape[1]
    dn = own[...] + from_left[...].astype(WIDE) + from_right[...].astype(WIDE)
    scale = lax.rsqrt(jnp.mean(x * x, -1, keepdims=True) + 1e-6)
    there = x * scale

    @pl.when(pl.program_id(0) == 0)
    def _():
        dg_s[...] = jnp.zeros_like(dg_s)

    dg_s[...] += (dn * there).reshape(-1, 8, d).sum(0)
    dh = dn * gain[...].astype(WIDE)
    dx = scale * (dh - there * jnp.mean(dh * there, -1, keepdims=True))
    dx_o[...] = (dx + dy[...].astype(WIDE)).astype(LOW)

    @pl.when(pl.program_id(0) == pl.num_programs(0) - 1)
    def _():
        dg_o[...] = dg_s[...].sum(0, keepdims=True)


def finish(own, from_left, from_right, x, dy, gain, step=128):
    rows, d = x.shape
    full = pl.BlockSpec((step, d), lambda i: (i, 0))
    return pl.pallas_call(
        _finish,
        grid=(rows // step,),
        in_specs=[full] * 5 + [_full(gain.shape)],
        out_specs=[full, _full((1, d))],
        out_shape=[_like((rows, d)), _like((1, d), WIDE)],
        scratch_shapes=[pltpu.VMEM((8, d), WIDE)],
        compiler_params=_params(),
        cost_estimate=_cost(20 * rows * d, [own, own, x, x, x]),
        name="finish",
    )(own, from_left, from_right, x, dy, gain)


def _total(part, out, got, send_sem, recv_sem, *, slots):
    me = lax.axis_index("tp")
    others = [lax.rem(me + s, slots) for s in range(1, slots)]
    barrier = pltpu.get_barrier_semaphore()
    for there in others:
        pl.semaphore_signal(barrier, inc=1, device_id={"tp": there}, device_id_type=pl.DeviceIdType.MESH)
    pl.semaphore_wait(barrier, slots - 1)
    sends = [pltpu.make_async_remote_copy(src_ref=part, dst_ref=got.at[slots - s], send_sem=send_sem.at[s], recv_sem=recv_sem.at[s],
                                          device_id={"tp": there}, device_id_type=pl.DeviceIdType.MESH) for s, there in enumerate(others, 1)]
    for copy in sends:
        copy.start()
    got[0] = part[...]
    for copy in sends:
        copy.wait()
    out[...] = sum(got[_slot(n, me, slots)] for n in range(slots))


def total(part, slots):
    copies = pltpu.SemaphoreType.DMA((slots,))
    return pl.pallas_call(
        functools.partial(_total, slots=slots),
        in_specs=[pl.BlockSpec(memory_space=pltpu.VMEM)],
        out_specs=pl.BlockSpec(memory_space=pltpu.VMEM),
        out_shape=_like(part.shape, WIDE),
        scratch_shapes=[pltpu.VMEM((slots, *part.shape), WIDE), copies, copies],
        compiler_params=_params(collective_id=2, has_side_effects=True),
        cost_estimate=_cost(slots * part.size, [part]),
        name="total",
    )(part)


def solution(mesh):
    slots = mesh.shape["tp"]
    right = [(i, (i + 1) % slots) for i in range(slots)]
    left = [(i, (i - 1) % slots) for i in range(slots)]

    def step(x, dy, gain, wq, wk, wv, wo):
        rows, d = x.shape
        gain_row = gain[None]
        half = HEAD // 2
        pace = jnp.tile(THETA ** (-jnp.arange(half, dtype=WIDE) / half), 2)[None]
        _, dys, a, dqkv, o = front(x, dy, gain_row, pace, wq, wk, wv, wo, slots)

        to_right, to_left, own = terms(dqkv, wq, wk, wv, slots)
        from_left, from_right = lax.ppermute(to_right, "tp", right), lax.ppermute(to_left, "tp", left)
        later, o, _ = lax.optimization_barrier((dqkv, o, to_right))
        dy_all = dys.reshape(-1, d)
        by_w = [lax.dot_general(a, t, (((0,), (0,)), ((), ())), preferred_element_type=WIDE).astype(LOW) for t in jnp.split(later, 3, 1)]
        by_wo = lax.dot_general(o, dy_all, (((0,), (0,)), ((), ())), preferred_element_type=WIDE).astype(LOW)
        by_x, by_gain = finish(own, from_left, from_right, x, dy, gain_row)
        return (by_x, total(by_gain, slots), *by_w, by_wo)

    tokens, columns = P(("dp", "tp"), None), P(None, "tp")
    return jax.shard_map(
        step,
        mesh=mesh,
        in_specs=(tokens, tokens, P(None), columns, columns, columns, P("tp", None)),
        out_specs=(tokens, P("dp", None), P("dp", "tp"), P("dp", "tp"), P("dp", "tp"), P(("dp", "tp"), None)),
        check_vma=False,
    )
```

```python
import functools

import jax
import jax.numpy as jnp
from jax import lax
from jax.experimental import pallas as pl
from jax.experimental.pallas import tpu as pltpu
from jax.sharding import PartitionSpec as P

HEAD = 128
THETA = 10000
NEG = -1e30
HIDDEN = 2 * NEG
LOG2E = 1.4426950408889634
VMEM = 58 * 2**20
LOW = jnp.bfloat16
WIDE = jnp.float32


def _dot(a, b, ca, cb):
    return lax.dot_general(a, b, (((ca,), (cb,)), ((), ())), preferred_element_type=WIDE)


def _params(**more):
    return pltpu.CompilerParams(vmem_limit_bytes=VMEM, **more)


def _cost(flops, arrays, exps=0):
    return pl.CostEstimate(flops=int(flops), transcendentals=int(exps), bytes_accessed=int(sum(a.size * a.dtype.itemsize for a in arrays)))


def _like(shape, dtype=LOW):
    return jax.ShapeDtypeStruct(shape, dtype)


ANY = pl.BlockSpec(memory_space=pl.ANY)


def _full(shape):
    return pl.BlockSpec(shape, lambda *_: (0,) * len(shape))


def _turn(t, cos, sin):
    return t * cos + pltpu.roll(t, HEAD // 2, 1) * sin


def _slot(block, me, slots):
    return lax.rem(block - me + slots, slots)


def _gap(keys, queries):
    return lax.broadcasted_iota(jnp.int32, (keys, queries), 1) - lax.broadcasted_iota(jnp.int32, (keys, queries), 0)


def _front(x, dy, gain, pace, wq, wk, wv, wo, xs, dys, a_o, d_o, o_o,
           wo_s, x_s, a_s, qkv_s, o_s, do_s, lse_s, gap_s, cos, sin, w_sem, x_sem, a_sem, out_sem, send_sem, recv_sem, *, slots, group):
    me = lax.axis_index("tp")
    rows, d = x.shape
    half, wide = rows // 2, wq.shape[1]
    heads = wide // HEAD
    right, left = lax.rem(me + 1, slots), lax.rem(me + slots - 1, slots)
    top, low = pl.ds(0, half), pl.ds(half, half)
    last = slots - 1
    scale = HEAD**-0.5
    e = scale * LOG2E

    barrier = pltpu.get_barrier_semaphore()
    for there in (left, right):
        pl.semaphore_signal(barrier, inc=1, device_id={"tp": there}, device_id_type=pl.DeviceIdType.MESH)
    pl.semaphore_wait(barrier, 2)

    def remote(n, src, dst, there):
        return pltpu.make_async_remote_copy(src_ref=src, dst_ref=dst, send_sem=send_sem.at[n], recv_sem=recv_sem.at[n],
                                            device_id={"tp": there}, device_id_type=pl.DeviceIdType.MESH)

    def transfers(n, t, ts):
        return [remote(n, t.at[top], ts.at[last, 0], right), remote(n + 1, t.at[low], ts.at[1, 1], left),
                remote(n + 2, t.at[low], ts.at[last, 1], right), remote(n + 3, t.at[top], ts.at[1, 0], left),
                remote(n + 4, ts.at[last, 0], ts.at[2, 0], right), remote(n + 5, ts.at[1, 1], ts.at[2, 1], left)]

    def start(copies):
        for copy in copies:
            copy.start()
        return copies

    def wait(copies):
        for copy in copies:
            copy.wait()

    def arrived(copies):
        for copy in copies:
            copy.wait_recv()

    x_go, dy_go = transfers(0, x, xs), transfers(6, dy, dys)
    start(x_go[:4])

    def into(ts, slot, p):
        return pltpu.make_async_copy(ts.at[slot, p], x_s.at[pl.ds(p * half, half)], x_sem.at[p])

    def own(t, p):
        return pltpu.make_async_copy(t.at[pl.ds(p * half, half)], x_s.at[pl.ds(p * half, half)], x_sem.at[p])

    def a_out(slot, p):
        return pltpu.make_async_copy(a_s.at[pl.ds(p * half, half)], a_o.at[pl.ds(slot * rows + p * half, half)], a_sem.at[p])

    loads = start([own(x, 0), own(x, 1)])
    wo_load = pltpu.make_async_copy(wo, wo_s, w_sem.at[3])
    gap_s[...] = _gap(rows, rows)

    def table(n, _):
        at = pl.ds(pl.multiple_of(n * 128, 128), 128)
        first = lax.rem(me + n * 128 // rows, slots) * rows + lax.rem(n * 128, rows)
        angle = (first + lax.broadcasted_iota(jnp.int32, (128, HEAD), 0)).astype(WIDE) * pace[...]
        cos[at, :] = jnp.cos(angle)
        sin[at, :] = jnp.where(lax.broadcasted_iota(jnp.int32, (128, HEAD), 1) < HEAD // 2, -1.0, 1.0) * jnp.sin(angle)

    lax.fori_loop(0, slots * rows // 128, table, None)
    g = gain[...].astype(WIDE)

    def by_seen(slot):
        at = slice(slot * rows, (slot + 1) * rows)

        for c in range(0, wide, 512):
            c = slice(c, min(c + 512, wide))
            do_s[at, c] = _dot(x_s[...], wo_s[c, :], 1, 1).astype(LOW)

    def head(n, h):
        return pl.ds(pl.multiple_of(n * wide + h * HEAD, HEAD), HEAD)

    def upward(w_s, top_s, mix_s):
        w_loads = start([pltpu.make_async_copy(w, w_s.at[:, pl.ds(i * wide, wide)], w_sem.at[i]) for i, w in enumerate((wq, wk, wv))])
        wo_load.start()
        top_s[...] = jnp.full_like(top_s, NEG)
        mix_s[...] = jnp.zeros_like(mix_s)

        def project(slot, parts, before):
            for p, earlier in zip(parts, before):
                if earlier is not None:
                    a_out(earlier, p).wait()
                for n in range(p * half, (p + 1) * half, 128):
                    t = x_s[n : n + 128, :].astype(WIDE)
                    size = lax.rsqrt(jnp.mean(t * t, -1, keepdims=True) + 1e-6)
                    a_s[n : n + 128, :] = (t * size * g).astype(LOW)
                a_out(slot, p).start()
            if slot == 0:
                wait(w_loads)
            first, count = parts[0] * half, len(parts) * half
            at, here = slice(slot * rows + first, slot * rows + first + count), slice(first, first + count)

            def turned(i, _):
                c = pl.ds(pl.multiple_of(i * 512, 512), 512)
                t = _dot(a_s[here, :], w_s[:, c], 1, 0).astype(LOW).astype(WIDE)
                qkv_s[at, c] = jnp.concatenate([_turn(t[:, h : h + HEAD], cos[at, :], sin[at, :]) for h in range(0, 512, HEAD)], 1).astype(LOW)

            lax.fori_loop(0, 2 * wide // 512, turned, None)
            for c in range(2 * wide, 3 * wide, 512):
                c = slice(c, min(c + 512, 3 * wide))
                qkv_s[at, c] = _dot(a_s[here, :], w_s[:, c], 1, 0).astype(LOW)

        def pair(sq, sk, masked, ks=(0, rows), qs=(0, rows)):
            mine, here = pl.ds(sq * rows + qs[0], qs[1] - qs[0]), pl.ds(sk * rows + ks[0], ks[1] - ks[0])
            to = slice(*qs)
            ones = jnp.ones((8, ks[1] - ks[0]), LOW)
            scores = [_dot(qkv_s[here, head(1, h)], qkv_s[mine, head(0, h)], 1, 1) for h in range(heads)]
            weights, keeps = [], []
            for h, s in enumerate(scores):
                if masked:
                    s = jnp.where(gap_s[slice(*ks), to] >= 0, s, HIDDEN)
                old = top_s[sq, h : h + 1, to]
                most = jnp.maximum(old, s.max(axis=0, keepdims=True))
                top_s[sq, h : h + 1, to] = most
                weights.append(jnp.exp2((s - most) * e).astype(LOW))
                keeps.append(jnp.exp2((old - most) * e))
            for h, (p, keep) in enumerate(zip(weights, keeps)):
                values = jnp.concatenate([qkv_s[here, head(2, h)].T, ones], axis=0)
                mix_s[sq, h, :, to] = mix_s[sq, h, :, to] * keep + _dot(values, p, 1, 0)

        wait(loads)
        project(0, (0, 1), (None, None))
        wait(start([own(dy, 0), own(dy, 1)]))
        keep = start([pltpu.make_async_copy(x_s.at[pl.ds(p * half, half)], dys.at[0, p], x_sem.at[p]) for p in range(2)])
        wo_load.wait()
        by_seen(0)
        wait(keep)
        arrived(x_go[:2])
        start(x_go[4:])
        wait(start([into(xs, last, 0), into(xs, 1, 1)]))
        project(last, (0,), (0,))
        project(1, (1,), (0,))
        arrived(x_go[2:4])
        start(dy_go[:4])
        wait(start([into(xs, 1, 0), into(xs, last, 1)]))
        project(1, (0,), (last,))
        project(last, (1,), (1,))

        def step(n, _):
            @pl.when(n == 9)
            def _():
                arrived(x_go[4:])
                wait(start([into(xs, 2, 0), into(xs, 2, 1)]))
                project(2, (0, 1), (1, last))

            i, j = n // 3, n % 3
            m = n - 9
            sq = jnp.where(n < 9, i + i // 2, jnp.where(m < 4, 2, m - 4 + (m - 4) // 2))
            sk = jnp.where(n < 9, j + j // 2, jnp.where(m < 4, m, 2))
            bq, bk = lax.rem(me + sq, slots), lax.rem(me + sk, slots)

            @pl.when(bk < bq)
            def _():
                pair(sq, sk, False)

            @pl.when(bk == bq)
            def _():
                pair(sq, sk, True, ks=(0, half))
                pair(sq, sk, True, ks=(half, rows), qs=(half, rows))

        lax.fori_loop(0, slots * slots, step, None)
        for slot in range(slots):
            for h in range(heads):
                total = mix_s[slot, h, HEAD : HEAD + 1, :]
                o_s[slot * rows : (slot + 1) * rows, head(0, h)] = (mix_s[slot, h, :HEAD, :] * (1 / total)).T.astype(LOW)
                lse_s[slot, h : h + 1, :] = top_s[slot, h : h + 1, :] * e + jnp.log2(total)
        wait([a_out(2, 0), a_out(2, 1)])

    pl.run_scoped(upward, pltpu.VMEM((d, 3 * wide), LOW), pltpu.VMEM((slots, heads, rows), WIDE),
                  pltpu.VMEM((slots, heads, HEAD + 8, rows), WIDE))
    o_out = start([pltpu.make_async_copy(o_s, o_o, w_sem.at[0])])
    arrived(dy_go[:2])
    start(dy_go[4:])

    def d_out(slot):
        at = pl.ds(slot * rows, rows)
        return pltpu.make_async_copy(qkv_s.at[at], d_o.at[at], out_sem.at[slot])

    def downward(dq_s, dk_s, dv_s):
        dk_s[...] = jnp.zeros_like(dk_s)
        dv_s[...] = jnp.zeros_like(dv_s)

        def step(n, _):
            @pl.when(n == 1)
            def _():
                arrived(dy_go[2:4])
                for slot in (1, last):
                    wait(start([into(dys, slot, 0), into(dys, slot, 1)]))
                    by_seen(slot)

            @pl.when(n == 3)
            def _():
                arrived(dy_go[4:])
                wait(start([into(dys, 2, 0), into(dys, 2, 1)]))
                by_seen(2)

            sq = jnp.where(n < 2, n, 5 - n)
            bq = lax.rem(me + sq, slots)
            mine = pl.ds(sq * rows, rows)

            def some(k, _):
                hs = [k * group + h for h in range(group)]
                cut = [head(0, h) for h in hs]
                dq_s[...] = jnp.zeros_like(dq_s)
                lses = [lse_s[sq, pl.ds(h, 1), :] for h in hs]
                deltas = [(do_s[mine, c].astype(WIDE) * o_s[mine, c].astype(WIDE)).T.sum(axis=0, keepdims=True) for c in cut]

                def block(j, masked, ks=(0, rows), qs=(0, rows)):
                    here = pl.ds(_slot(j, me, slots) * rows + ks[0], ks[1] - ks[0])
                    there, to = pl.ds(sq * rows + qs[0], qs[1] - qs[0]), slice(*qs)
                    scores = [_dot(qkv_s[here, head(1, h)], qkv_s[there, head(0, h)], 1, 1) for h in hs]
                    dps = [_dot(qkv_s[here, head(2, h)], do_s[there, c], 1, 1) for h, c in zip(hs, cut)]
                    for i, (h, c) in enumerate(zip(hs, cut)):
                        p = jnp.exp2(scores[i] * e - lses[i][:, to])
                        if masked:
                            p = jnp.where(gap_s[slice(*ks), to] >= 0, p, 0.0)
                        ds = (p * (dps[i] - deltas[i][:, to])).astype(LOW)
                        dv_s[here, c] += _dot(p.astype(LOW), do_s[there, c], 1, 0)
                        dk_s[here, c] += _dot(ds, qkv_s[there, c], 1, 0)
                        dq_s[i, :, to] += _dot(qkv_s[here, head(1, h)].T, ds, 1, 0)

                lax.fori_loop(0, bq, lambda j, _: block(j, False), None)
                block(bq, True, ks=(0, half))
                block(bq, True, ks=(half, rows), qs=(half, rows))
                for i, c in enumerate(cut):
                    dq = (dq_s[i] * scale).T.astype(LOW).astype(WIDE)
                    qkv_s[mine, c] = _turn(dq, cos[mine, :], -sin[mine, :]).astype(LOW)

            lax.fori_loop(0, heads // group, some, None)

        lax.fori_loop(0, slots, step, None)

        def finish(slot, _):
            at = pl.ds(slot * rows, rows)
            for h in range(heads):
                c = head(0, h)
                dk = (dk_s[at, c] * scale).astype(LOW).astype(WIDE)
                qkv_s[at, head(1, h)] = _turn(dk, cos[at, :], -sin[at, :]).astype(LOW)
                qkv_s[at, head(2, h)] = dv_s[at, c].astype(LOW)
            d_out(slot).start()

        lax.fori_loop(0, slots, finish, None)

    pl.run_scoped(downward, pltpu.VMEM((group, HEAD, rows), WIDE), pltpu.VMEM((slots * rows, wide), WIDE),
                  pltpu.VMEM((slots * rows, wide), WIDE))
    wait(o_out)
    wait([d_out(slot) for slot in range(slots)])
    for copy in (*x_go, *dy_go):
        copy.wait_send()


def front(x, dy, gain, pace, wq, wk, wv, wo, slots, group=3):
    rows, d = x.shape
    wide = wq.shape[1]
    total, heads = slots * rows, wide // HEAD
    blocks = _like((slots, 2, rows // 2, d))
    copies = pltpu.SemaphoreType.DMA((12,))
    return pl.pallas_call(
        functools.partial(_front, slots=slots, group=group),
        in_specs=[ANY, ANY] + [pl.BlockSpec(memory_space=pltpu.VMEM)] * 2 + [ANY] * 4,
        out_specs=[ANY] * 5,
        out_shape=[blocks, blocks, _like((total, d)), _like((total, 3 * wide)), _like((total, wide))],
        scratch_shapes=[pltpu.VMEM((wide, d), LOW), pltpu.VMEM((rows, d), LOW), pltpu.VMEM((rows, d), LOW),
                        pltpu.VMEM((total, 3 * wide), LOW), pltpu.VMEM((total, wide), LOW), pltpu.VMEM((total, wide), LOW),
                        pltpu.VMEM((slots, heads, rows), WIDE), pltpu.VMEM((rows, rows), jnp.int32),
                        pltpu.VMEM((total, HEAD), WIDE), pltpu.VMEM((total, HEAD), WIDE), pltpu.SemaphoreType.DMA((4,)), pltpu.SemaphoreType.DMA((2,)), pltpu.SemaphoreType.DMA((2,)),
                        pltpu.SemaphoreType.DMA((slots,)), copies, copies],
        compiler_params=_params(collective_id=0, has_side_effects=True),
        cost_estimate=_cost(2 * total * d * 4 * wide + 14 * total * total * wide, [x] * 20, 2 * total * total * heads),
        name="front",
    )(x, dy, gain, pace, wq, wk, wv, wo)


def _terms(d_i, wq, wk, wv, right_o, left_o, own_o, d_s, w_s, far_s, got_s, wide_s, low_s, own_s, w_sem, d_sem, out_sem, send_sem, recv_sem, *, slots):
    me = lax.axis_index("tp")
    rows, d = own_o.shape
    wide = wq.shape[1]
    right, left = lax.rem(me + 1, slots), lax.rem(me + slots - 1, slots)
    last, half, tile = slots - 1, d // 2, d // 4
    tiles = 4

    def d_in(slot):
        return pltpu.make_async_copy(d_i.at[pl.ds(slot * rows, rows)], d_s.at[slot], d_sem.at[slot])

    def w_in(i, n):
        return pltpu.make_async_copy((wq, wk, wv)[i].at[pl.ds(n * tile, tile)], w_s.at[pl.ds(n * tile, tile), pl.ds(i * wide, wide)], w_sem.at[i, n])

    d_in(2).start()
    for n in range(tiles):
        for i in range(3):
            w_in(i, n).start()
    for slot in (1, last, 0):
        d_in(slot).start()
    barrier = pltpu.get_barrier_semaphore()
    for there in (left, right):
        pl.semaphore_signal(barrier, inc=1, device_id={"tp": there}, device_id_type=pl.DeviceIdType.MESH)
    pl.semaphore_wait(barrier, 2)
    sends = [pltpu.make_async_remote_copy(src_ref=far_s.at[p], dst_ref=got_s.at[p], send_sem=send_sem.at[p], recv_sem=recv_sem.at[p],
                                          device_id={"tp": there}, device_id_type=pl.DeviceIdType.MESH) for p, there in enumerate((right, left) * 2)]

    def columns(n):
        return pl.ds(pl.multiple_of(n * tile, tile), tile)

    def term(slot, n):
        return _dot(d_s[slot], w_s[columns(n), :], 1, 1)

    d_in(2).wait()

    def far(n, _):
        m = n % 2 * 2 + n // 2
        for i in range(3):
            w_in(i, m).wait()
        far_s[n] = term(2, m).astype(LOW)
        for i in range(1, tiles):

            @pl.when(n == i)
            def _():
                sends[i - 1].start()

    lax.fori_loop(0, tiles, far, None)
    for slot in (1, last, 0):
        d_in(slot).wait()

    def near(n, _):
        m = n + tiles // 2
        low_s[0, :, columns(m)] = term(1, m).astype(LOW)

        @pl.when(n == 0)
        def _():
            sends[tiles - 1].start()

        low_s[1, :, columns(n)] = term(last, n).astype(LOW)
        wide_s[0, :, columns(n)] = term(1, n)
        wide_s[1, :, columns(n)] = term(last, m)

    lax.fori_loop(0, tiles // 2, near, None)

    def own(n, _):
        own_s[:, columns(n)] = term(0, n)

    lax.fori_loop(0, tiles, own, None)
    own_out = pltpu.make_async_copy(own_s, own_o, out_sem.at[2])
    own_out.start()
    for i, copy in enumerate(sends):
        copy.wait_recv()
        p, n = i % 2, i // 2
        from_, to = slice(n * tile, (n + 1) * tile), slice(p * half + n * tile, p * half + (n + 1) * tile)

        def add(r, _):
            at = pl.ds(pl.multiple_of(r * 128, 128), 128)
            low_s[p, at, to] = (wide_s[p, at, from_] + got_s[i, at, :].astype(WIDE)).astype(LOW)

        lax.fori_loop(0, rows // 128, add, None)
    outs = [pltpu.make_async_copy(low_s.at[p], o, out_sem.at[p]) for p, o in enumerate((right_o, left_o))]
    for copy in outs:
        copy.start()
    for copy in (*outs, own_out):
        copy.wait()
    for copy in sends:
        copy.wait_send()


def terms(dqkv, wq, wk, wv, slots):
    d, wide = wq.shape
    rows = dqkv.shape[0] // slots
    four = pltpu.SemaphoreType.DMA((4,))
    return pl.pallas_call(
        functools.partial(_terms, slots=slots),
        in_specs=[ANY] * 4,
        out_specs=[ANY] * 3,
        out_shape=[_like((rows, d)), _like((rows, d)), _like((rows, d), WIDE)],
        scratch_shapes=[pltpu.VMEM((slots, rows, 3 * wide), LOW), pltpu.VMEM((d, 3 * wide), LOW), pltpu.VMEM((4, rows, d // 4), LOW),
                        pltpu.VMEM((4, rows, d // 4), LOW), pltpu.VMEM((2, rows, d // 2), WIDE), pltpu.VMEM((2, rows, d), LOW),
                        pltpu.VMEM((rows, d), WIDE), pltpu.SemaphoreType.DMA((3, 4)), pltpu.SemaphoreType.DMA((slots,)),
                        pltpu.SemaphoreType.DMA((3,)), four, four],
        compiler_params=_params(collective_id=1, has_side_effects=True),
        cost_estimate=_cost(6 * slots * rows * d * wide, [dqkv, wq, wk, wv]),
        name="terms",
    )(dqkv, wq, wk, wv)


def _finish(own, x, dy, from_left, from_right, gain, dx_o, dg_o, dn_s, part_s, got_s, send_sem, recv_sem, *, slots, step):
    me = lax.axis_index("tp")
    rows, d = x.shape
    others = [lax.rem(me + s, slots) for s in range(1, slots)]
    barrier = pltpu.get_barrier_semaphore()
    for there in others:
        pl.semaphore_signal(barrier, inc=1, device_id={"tp": there}, device_id_type=pl.DeviceIdType.MESH)
    pl.semaphore_wait(barrier, slots - 1)
    g = gain[...].astype(WIDE)
    part_s[...] = jnp.zeros_like(part_s)

    def first(n, _):
        at = pl.ds(pl.multiple_of(n * step, step), step)
        t = x[at, :].astype(WIDE)
        dn = own[at, :] + from_left[at, :].astype(WIDE) + from_right[at, :].astype(WIDE)
        dn_s[at, :] = dn
        part_s[...] += (dn * (t * lax.rsqrt(jnp.mean(t * t, -1, keepdims=True) + 1e-6))).reshape(-1, 8, d).sum(0)

    lax.fori_loop(0, rows // step, first, None)
    sends = [pltpu.make_async_remote_copy(src_ref=part_s, dst_ref=got_s.at[slots - s], send_sem=send_sem.at[s], recv_sem=recv_sem.at[s],
                                          device_id={"tp": there}, device_id_type=pl.DeviceIdType.MESH) for s, there in enumerate(others, 1)]

    def second(n, _):
        at = pl.ds(pl.multiple_of(n * step, step), step)
        t = x[at, :].astype(WIDE)
        size = lax.rsqrt(jnp.mean(t * t, -1, keepdims=True) + 1e-6)
        there = t * size
        dh = dn_s[at, :] * g
        dx = size * (dh - there * jnp.mean(dh * there, -1, keepdims=True))
        dx_o[at, :] = (dx + dy[at, :].astype(WIDE)).astype(LOW)

        @pl.when(n == 0)
        def _():
            for copy in sends:
                copy.start()

    lax.fori_loop(0, rows // step, second, None)
    got_s[0] = part_s[...]
    for copy in sends:
        copy.wait()
    dg_o[...] = sum(got_s[_slot(n, me, slots)] for n in range(slots)).sum(0, keepdims=True)


def finish(own, from_left, from_right, x, dy, gain, slots, step=64):
    rows, d = x.shape
    copies = pltpu.SemaphoreType.DMA((slots,))
    here = pl.BlockSpec(memory_space=pltpu.VMEM)
    return pl.pallas_call(
        functools.partial(_finish, slots=slots, step=step),
        in_specs=[here] * 6,
        out_specs=[here] * 2,
        out_shape=[_like((rows, d)), _like((1, d), WIDE)],
        scratch_shapes=[pltpu.VMEM((rows, d), WIDE), pltpu.VMEM((8, d), WIDE), pltpu.VMEM((slots, 8, d), WIDE), copies, copies],
        compiler_params=pltpu.CompilerParams(vmem_limit_bytes=24 * 2**20, collective_id=2, has_side_effects=True),
        cost_estimate=_cost(20 * rows * d, [own, own, x, x, x]),
        name="finish",
    )(own, x, dy, from_left, from_right, gain)


def solution(mesh):
    slots = mesh.shape["tp"]
    right = [(i, (i + 1) % slots) for i in range(slots)]
    left = [(i, (i - 1) % slots) for i in range(slots)]

    def step(x, dy, gain, wq, wk, wv, wo):
        rows, d = x.shape
        gain_row = gain[None]
        half = HEAD // 2
        pace = jnp.tile(THETA ** (-jnp.arange(half, dtype=WIDE) / half), 2)[None]
        _, dys, a, dqkv, o = front(x, dy, gain_row, pace, wq, wk, wv, wo, slots)

        to_right, to_left, own = terms(dqkv, wq, wk, wv, slots)
        from_left, from_right = lax.ppermute(to_right, "tp", right), lax.ppermute(to_left, "tp", left)
        later, o, _ = lax.optimization_barrier((dqkv, o, to_right))
        dy_all = dys.reshape(-1, d)
        by_w = [lax.dot_general(a, t, (((0,), (0,)), ((), ())), preferred_element_type=WIDE).astype(LOW) for t in jnp.split(later, 3, 1)]
        by_wo = lax.dot_general(o, dy_all, (((0,), (0,)), ((), ())), preferred_element_type=WIDE).astype(LOW)
        return (*finish(own, from_left, from_right, x, dy, gain_row, slots), *by_w, by_wo)

    tokens, columns = P(("dp", "tp"), None), P(None, "tp")
    return jax.shard_map(
        step,
        mesh=mesh,
        in_specs=(tokens, tokens, P(None), columns, columns, columns, P("tp", None)),
        out_specs=(tokens, P("dp", None), P("dp", "tp"), P("dp", "tp"), P("dp", "tp"), P(("dp", "tp"), None)),
        check_vma=False,
    )
```

```python
import functools

import jax
import jax.numpy as jnp
import numpy as np
from jax import lax
from jax.experimental import pallas as pl
from jax.experimental.pallas import tpu as pltpu
from jax.sharding import PartitionSpec as P

HEAD = 128
THETA = 10000
NEG = -1e30
HIDDEN = 2 * NEG
LOG2E = 1.4426950408889634
VMEM = 63 * 2**20
LOW = jnp.bfloat16
WIDE = jnp.float32


def _dot(a, b, ca, cb):
    return lax.dot_general(a, b, (((ca,), (cb,)), ((), ())), preferred_element_type=WIDE)


def _params(**more):
    return pltpu.CompilerParams(vmem_limit_bytes=VMEM, **more)


def _cost(flops, arrays, exps=0):
    return pl.CostEstimate(flops=int(flops), transcendentals=int(exps), bytes_accessed=int(sum(a.size * a.dtype.itemsize for a in arrays)))


def _like(shape, dtype=LOW):
    return jax.ShapeDtypeStruct(shape, dtype)


ANY = pl.BlockSpec(memory_space=pl.ANY)


def _full(shape):
    return pl.BlockSpec(shape, lambda *_: (0,) * len(shape))


def _turn(t, cos, sin):
    return t * cos + pltpu.roll(t, HEAD // 2, 1) * sin


def _slot(block, me, slots):
    return lax.rem(block - me + slots, slots)


def _gap(keys, queries):
    return lax.broadcasted_iota(jnp.int32, (keys, queries), 1) - lax.broadcasted_iota(jnp.int32, (keys, queries), 0)


def _front(x, dy, gain, pace, wq, wk, wv, wo, xs, dys, a_o, d_o, o_o, right_o, left_o, own_o,
           wo_s, x_s, a_s, qkv_s, o_s, do_s, lse_s, gap_s, cos, sin, got_s, w_sem, x_sem, a_sem, out_sem, term_sem, send_sem, recv_sem,
           *, slots, group):
    me = lax.axis_index("tp")
    rows, d = x.shape
    half, wide = rows // 2, wq.shape[1]
    heads = wide // HEAD
    right, left = lax.rem(me + 1, slots), lax.rem(me + slots - 1, slots)
    top, low = pl.ds(0, half), pl.ds(half, half)
    last = slots - 1
    scale = HEAD**-0.5
    e = scale * LOG2E

    barrier = pltpu.get_barrier_semaphore()
    for there in (left, right):
        pl.semaphore_signal(barrier, inc=1, device_id={"tp": there}, device_id_type=pl.DeviceIdType.MESH)
    pl.semaphore_wait(barrier, 2)

    def remote(n, src, dst, there):
        return pltpu.make_async_remote_copy(src_ref=src, dst_ref=dst, send_sem=send_sem.at[n], recv_sem=recv_sem.at[n],
                                            device_id={"tp": there}, device_id_type=pl.DeviceIdType.MESH)

    def transfers(n, t, ts):
        return [remote(n, t.at[top], ts.at[last, 0], right), remote(n + 1, t.at[low], ts.at[1, 1], left),
                remote(n + 2, t.at[low], ts.at[last, 1], right), remote(n + 3, t.at[top], ts.at[1, 0], left),
                remote(n + 4, ts.at[last, 0], ts.at[2, 0], right), remote(n + 5, ts.at[1, 1], ts.at[2, 1], left)]

    def start(copies):
        for copy in copies:
            copy.start()
        return copies

    def wait(copies):
        for copy in copies:
            copy.wait()

    def arrived(copies):
        for copy in copies:
            copy.wait_recv()

    x_go, dy_go = transfers(0, x, xs), transfers(6, dy, dys)
    start(x_go[:4])

    def into(ts, slot, p):
        return pltpu.make_async_copy(ts.at[slot, p], x_s.at[pl.ds(p * half, half)], x_sem.at[p])

    def own(t, p):
        return pltpu.make_async_copy(t.at[pl.ds(p * half, half)], x_s.at[pl.ds(p * half, half)], x_sem.at[p])

    def a_out(slot, p):
        return pltpu.make_async_copy(a_s.at[pl.ds(p * half, half)], a_o.at[pl.ds(slot * rows + p * half, half)], a_sem.at[p])

    loads = start([own(x, 0), own(x, 1)])
    wo_load = pltpu.make_async_copy(wo, wo_s, w_sem.at[3])
    gap_s[...] = _gap(rows, rows)

    def table(n, _):
        at = pl.ds(pl.multiple_of(n * 128, 128), 128)
        first = lax.rem(me + n * 128 // rows, slots) * rows + lax.rem(n * 128, rows)
        angle = (first + lax.broadcasted_iota(jnp.int32, (128, HEAD), 0)).astype(WIDE) * pace[...]
        cos[at, :] = jnp.cos(angle)
        sin[at, :] = jnp.where(lax.broadcasted_iota(jnp.int32, (128, HEAD), 1) < HEAD // 2, -1.0, 1.0) * jnp.sin(angle)

    lax.fori_loop(0, slots * rows // 128, table, None)
    g = gain[...].astype(WIDE).reshape(1, d)

    def by_seen(slot):
        at = slice(slot * rows, (slot + 1) * rows)

        for c in range(0, wide, 512):
            c = slice(c, min(c + 512, wide))
            do_s[at, c] = _dot(x_s[...], wo_s[c, :], 1, 1).astype(LOW)

    def head(n, h):
        return pl.ds(pl.multiple_of(n * wide + h * HEAD, HEAD), HEAD)

    def upward(w_s, top_s, mix_s):
        w_loads = start([pltpu.make_async_copy(w, w_s.at[:, pl.ds(i * wide, wide)], w_sem.at[i]) for i, w in enumerate((wq, wk, wv))])
        wo_load.start()
        top_s[...] = jnp.full_like(top_s, NEG)
        mix_s[...] = jnp.zeros_like(mix_s)

        def project(slot, parts, before):
            for p, earlier in zip(parts, before):
                if earlier is not None:
                    a_out(earlier, p).wait()
                for n in range(p * half, (p + 1) * half, 128):
                    t = x_s[n : n + 128, :].astype(WIDE)
                    size = lax.rsqrt(jnp.mean(t * t, -1, keepdims=True) + 1e-6)
                    a_s[n : n + 128, :] = (t * size * g).astype(LOW)
                a_out(slot, p).start()
            if slot == 0:
                wait(w_loads)
            first, count = parts[0] * half, len(parts) * half
            at, here = slice(slot * rows + first, slot * rows + first + count), slice(first, first + count)

            def turned(i, _):
                c = pl.ds(pl.multiple_of(i * 512, 512), 512)
                t = _dot(a_s[here, :], w_s[:, c], 1, 0).astype(LOW).astype(WIDE)
                qkv_s[at, c] = jnp.concatenate([_turn(t[:, h : h + HEAD], cos[at, :], sin[at, :]) for h in range(0, 512, HEAD)], 1).astype(LOW)

            lax.fori_loop(0, 2 * wide // 512, turned, None)
            for c in range(2 * wide, 3 * wide, 512):
                c = slice(c, min(c + 512, 3 * wide))
                qkv_s[at, c] = _dot(a_s[here, :], w_s[:, c], 1, 0).astype(LOW)

        def pair(sq, sk, masked, ks=(0, rows), qs=(0, rows)):
            mine, here = pl.ds(sq * rows + qs[0], qs[1] - qs[0]), pl.ds(sk * rows + ks[0], ks[1] - ks[0])
            to = slice(*qs)
            ones = jnp.ones((8, ks[1] - ks[0]), LOW)

            def some(k, _):
                hs = [k * group + h for h in range(group)]
                scores = [_dot(qkv_s[here, head(1, h)], qkv_s[mine, head(0, h)], 1, 1) for h in hs]
                weights, keeps = [], []
                for h, s in zip(hs, scores):
                    if masked:
                        s = jnp.where(gap_s[slice(*ks), to] >= 0, s, HIDDEN)
                    old = top_s[sq, pl.ds(h, 1), to]
                    most = jnp.maximum(old, s.max(axis=0, keepdims=True))
                    top_s[sq, pl.ds(h, 1), to] = most
                    weights.append(jnp.exp2((s - most) * e).astype(LOW))
                    keeps.append(jnp.exp2((old - most) * e))
                for h, p, keep in zip(hs, weights, keeps):
                    values = jnp.concatenate([qkv_s[here, head(2, h)].T, ones], axis=0)
                    mix_s[sq, h, :, to] = mix_s[sq, h, :, to] * keep + _dot(values, p, 1, 0)

            lax.fori_loop(0, heads // group, some, None)

        wait(loads)
        project(0, (0, 1), (None, None))
        wait(start([own(dy, 0), own(dy, 1)]))
        keep = start([pltpu.make_async_copy(x_s.at[pl.ds(p * half, half)], dys.at[0, p], x_sem.at[p]) for p in range(2)])
        wo_load.wait()
        by_seen(0)
        wait(keep)
        arrived(x_go[:2])
        start(x_go[4:])
        wait(start([into(xs, last, 0), into(xs, 1, 1)]))
        project(last, (0,), (0,))
        project(1, (1,), (0,))
        arrived(x_go[2:4])
        start(dy_go[:4])
        wait(start([into(xs, 1, 0), into(xs, last, 1)]))
        project(1, (0,), (last,))
        project(last, (1,), (1,))

        def step(n, _):
            @pl.when(n == 9)
            def _():
                arrived(x_go[4:])
                wait(start([into(xs, 2, 0), into(xs, 2, 1)]))
                project(2, (0, 1), (1, last))

            i, j = n // 3, n % 3
            m = n - 9
            sq = jnp.where(n < 9, i + i // 2, jnp.where(m < 4, 2, m - 4 + (m - 4) // 2))
            sk = jnp.where(n < 9, j + j // 2, jnp.where(m < 4, m, 2))
            bq, bk = lax.rem(me + sq, slots), lax.rem(me + sk, slots)

            @pl.when(bk < bq)
            def _():
                pair(sq, sk, False)

            @pl.when(bk == bq)
            def _():
                pair(sq, sk, True, ks=(0, half))
                pair(sq, sk, True, ks=(half, rows), qs=(half, rows))

        lax.fori_loop(0, slots * slots, step, None)

        def settle(slot, _):
            at = pl.ds(slot * rows, rows)
            for h in range(heads):
                total = mix_s[slot, h, HEAD : HEAD + 1, :]
                o_s[at, head(0, h)] = (mix_s[slot, h, :HEAD, :] * (1 / total)).T.astype(LOW)
                lse_s[slot, h : h + 1, :] = top_s[slot, h : h + 1, :] * e + jnp.log2(total)

        lax.fori_loop(0, slots, settle, None)
        wait([a_out(2, 0), a_out(2, 1)])

    pl.run_scoped(upward, pltpu.VMEM((d, 3 * wide), LOW), pltpu.VMEM((slots, heads, rows), WIDE),
                  pltpu.VMEM((slots, heads, HEAD + 8, rows), WIDE))
    o_out = start([pltpu.make_async_copy(o_s, o_o, w_sem.at[0])])
    arrived(dy_go[:2])
    start(dy_go[4:])

    def d_out(slot):
        at = pl.ds(slot * rows, rows)
        return pltpu.make_async_copy(qkv_s.at[at], d_o.at[at], out_sem.at[slot])

    def downward(w_s, dq_s, dk_s, dv_s):
        dk_s[...] = jnp.zeros_like(dk_s)
        dv_s[...] = jnp.zeros_like(dv_s)

        def step(n, _):
            @pl.when(n == 1)
            def _():
                arrived(dy_go[2:4])
                for slot in (1, last):
                    wait(start([into(dys, slot, 0), into(dys, slot, 1)]))
                    by_seen(slot)

            @pl.when(n == 3)
            def _():
                arrived(dy_go[4:])
                wait(start([into(dys, 2, 0), into(dys, 2, 1)]))
                by_seen(2)

            sq = jnp.where(n < 2, n, 5 - n)
            bq = lax.rem(me + sq, slots)
            mine = pl.ds(sq * rows, rows)

            def some(k, _):
                hs = [k * group + h for h in range(group)]
                cut = [head(0, h) for h in hs]
                dq_s[...] = jnp.zeros_like(dq_s)
                lses = [lse_s[sq, pl.ds(h, 1), :] for h in hs]
                deltas = [(do_s[mine, c].astype(WIDE) * o_s[mine, c].astype(WIDE)).T.sum(axis=0, keepdims=True) for c in cut]

                def block(j, masked, ks=(0, rows), qs=(0, rows)):
                    here = pl.ds(_slot(j, me, slots) * rows + ks[0], ks[1] - ks[0])
                    there, to = pl.ds(sq * rows + qs[0], qs[1] - qs[0]), slice(*qs)
                    scores = [_dot(qkv_s[here, head(1, h)], qkv_s[there, head(0, h)], 1, 1) for h in hs]
                    dps = [_dot(qkv_s[here, head(2, h)], do_s[there, c], 1, 1) for h, c in zip(hs, cut)]
                    for i, (h, c) in enumerate(zip(hs, cut)):
                        p = jnp.exp2(scores[i] * e - lses[i][:, to])
                        if masked:
                            p = jnp.where(gap_s[slice(*ks), to] >= 0, p, 0.0)
                        ds = (p * (dps[i] - deltas[i][:, to])).astype(LOW)
                        dv_s[here, c] += _dot(p.astype(LOW), do_s[there, c], 1, 0)
                        dk_s[here, c] += _dot(ds, qkv_s[there, c], 1, 0)
                        dq_s[i, :, to] += _dot(qkv_s[here, head(1, h)].T, ds, 1, 0)

                lax.fori_loop(0, bq, lambda j, _: block(j, False), None)
                block(bq, True, ks=(0, half))
                block(bq, True, ks=(half, rows), qs=(half, rows))
                for i, c in enumerate(cut):
                    dq = (dq_s[i] * scale).T.astype(LOW).astype(WIDE)
                    qkv_s[mine, c] = _turn(dq, cos[mine, :], -sin[mine, :]).astype(LOW)

            lax.fori_loop(0, heads // group, some, None)

        lax.fori_loop(0, slots, step, None)

        def settle(slot, _):
            at = pl.ds(slot * rows, rows)
            for h in range(heads):
                c = head(0, h)
                dk = (dk_s[at, c] * scale).astype(LOW).astype(WIDE)
                qkv_s[at, head(1, h)] = _turn(dk, cos[at, :], -sin[at, :]).astype(LOW)
                qkv_s[at, head(2, h)] = dv_s[at, c].astype(LOW)
            d_out(slot).start()

        settle(2, None)
        wait(w_in(w_s))

        def far(n, _):
            m = n % 2 * 2 + n // 2
            x_s[:, columns(m)] = term(w_s, 2, m).astype(LOW)
            for i in range(1, tiles):

                @pl.when(n == i)
                def _():
                    far_go[i - 1].start()

        lax.fori_loop(0, tiles, far, None)
        lax.fori_loop(0, slots - 1, lambda n, _: settle(n + n // 2, None), None)

    def across(w_s, low_s, wide_s, own_s):
        def near(n, _):
            m = n + tiles // 2
            low_s[0, :, columns(m)] = term(w_s, 1, m).astype(LOW)
            low_s[1, :, columns(n)] = term(w_s, last, n).astype(LOW)
            wide_s[0, :, columns(n)] = term(w_s, 1, n)
            wide_s[1, :, columns(n)] = term(w_s, last, m)

        far_go[tiles - 1].start()
        lax.fori_loop(0, tiles // 2, near, None)

        def own(n, _):
            own_s[:, columns(n)] = term(w_s, 0, n)

        lax.fori_loop(0, tiles, own, None)
        own_out = start([pltpu.make_async_copy(own_s, own_o, term_sem.at[2])])
        for i, copy in enumerate(far_go):
            copy.wait_recv()
            p, n = i % 2, i // 2
            from_, to = slice(n * tile, (n + 1) * tile), slice((p * 2 + n) * tile, (p * 2 + n + 1) * tile)

            def add(r, _):
                at = pl.ds(pl.multiple_of(r * 128, 128), 128)
                low_s[p, at, to] = (wide_s[p, at, from_] + got_s[i, at, :].astype(WIDE)).astype(LOW)

            lax.fori_loop(0, rows // 128, add, None)
        wait(start([pltpu.make_async_copy(low_s.at[p], o, term_sem.at[p]) for p, o in enumerate((right_o, left_o))]))
        wait(own_out)

    tiles, tile = 4, d // 4
    far_go = [remote(12 + i, x_s.at[:, pl.ds((i % 2 * 2 + i // 2) * tile, tile)], got_s.at[i], (right, left)[i % 2]) for i in range(tiles)]

    def columns(n):
        return pl.ds(pl.multiple_of(n * tile, tile), tile)

    def term(w_s, slot, n):
        return _dot(qkv_s[slot * rows : (slot + 1) * rows, :], w_s[columns(n), :], 1, 1)

    def w_in(w_s):
        return [pltpu.make_async_copy(w, w_s.at[:, pl.ds(i * wide, wide)], w_sem.at[1 + i]) for i, w in enumerate((wq, wk, wv))]

    def downward_and_across(w_s):
        start(w_in(w_s))
        pl.run_scoped(functools.partial(downward, w_s), pltpu.VMEM((group, HEAD, rows), WIDE), pltpu.VMEM((slots * rows, wide), WIDE),
                      pltpu.VMEM((slots * rows, wide), WIDE))
        pl.run_scoped(functools.partial(across, w_s), pltpu.VMEM((2, rows, d), LOW), pltpu.VMEM((2, rows, d // 2), WIDE),
                      pltpu.VMEM((rows, d), WIDE))

    pl.run_scoped(downward_and_across, pltpu.VMEM((d, 3 * wide), LOW))
    wait(o_out)
    wait([d_out(slot) for slot in range(slots)])
    for copy in (*x_go, *dy_go, *far_go):
        copy.wait_send()


def front(x, dy, gain, pace, wq, wk, wv, wo, slots, group=3):
    rows, d = x.shape
    wide = wq.shape[1]
    total, heads = slots * rows, wide // HEAD
    blocks = _like((slots, 2, rows // 2, d))
    copies = pltpu.SemaphoreType.DMA((16,))
    return pl.pallas_call(
        functools.partial(_front, slots=slots, group=group),
        in_specs=[ANY, ANY] + [pl.BlockSpec(memory_space=pltpu.VMEM)] * 2 + [ANY] * 4,
        out_specs=[ANY] * 8,
        out_shape=[blocks, blocks, _like((total, d)), _like((total, 3 * wide)), _like((total, wide)), _like((rows, d)), _like((rows, d)),
                   _like((rows, d), WIDE)],
        scratch_shapes=[pltpu.VMEM((wide, d), LOW), pltpu.VMEM((rows, d), LOW), pltpu.VMEM((rows, d), LOW),
                        pltpu.VMEM((total, 3 * wide), LOW), pltpu.VMEM((total, wide), LOW), pltpu.VMEM((total, wide), LOW),
                        pltpu.VMEM((slots, heads, rows), WIDE), pltpu.VMEM((rows, rows), jnp.int32),
                        pltpu.VMEM((total, HEAD), WIDE), pltpu.VMEM((total, HEAD), WIDE), pltpu.VMEM((4, rows, d // 4), LOW),
                        pltpu.SemaphoreType.DMA((4,)), pltpu.SemaphoreType.DMA((2,)), pltpu.SemaphoreType.DMA((2,)),
                        pltpu.SemaphoreType.DMA((slots,)), pltpu.SemaphoreType.DMA((3,)), copies, copies],
        compiler_params=_params(collective_id=0, has_side_effects=True),
        cost_estimate=_cost(2 * total * d * 7 * wide + 14 * total * total * wide, [x] * 20, 2 * total * total * heads),
        name="front",
    )(x, dy, gain, pace, wq, wk, wv, wo)


def _finish(own, x, dy, from_left, from_right, gain, dx_o, dg_o, dn_s, part_s, got_s, send_sem, recv_sem, *, slots, step):
    me = lax.axis_index("tp")
    rows, d = x.shape
    others = [lax.rem(me + s, slots) for s in range(1, slots)]
    barrier = pltpu.get_barrier_semaphore()
    for there in others:
        pl.semaphore_signal(barrier, inc=1, device_id={"tp": there}, device_id_type=pl.DeviceIdType.MESH)
    pl.semaphore_wait(barrier, slots - 1)
    g = gain[...].astype(WIDE)
    part_s[...] = jnp.zeros_like(part_s)

    def first(n, _):
        at = pl.ds(pl.multiple_of(n * step, step), step)
        t = x[at, :].astype(WIDE)
        dn = own[at, :] + from_left[at, :].astype(WIDE) + from_right[at, :].astype(WIDE)
        dn_s[at, :] = dn
        part_s[...] += (dn * (t * lax.rsqrt(jnp.mean(t * t, -1, keepdims=True) + 1e-6))).reshape(-1, 8, d).sum(0)

    lax.fori_loop(0, rows // step, first, None)
    sends = [pltpu.make_async_remote_copy(src_ref=part_s, dst_ref=got_s.at[slots - s], send_sem=send_sem.at[s], recv_sem=recv_sem.at[s],
                                          device_id={"tp": there}, device_id_type=pl.DeviceIdType.MESH) for s, there in enumerate(others, 1)]

    def second(n, _):
        at = pl.ds(pl.multiple_of(n * step, step), step)
        t = x[at, :].astype(WIDE)
        size = lax.rsqrt(jnp.mean(t * t, -1, keepdims=True) + 1e-6)
        there = t * size
        dh = dn_s[at, :] * g
        dx = size * (dh - there * jnp.mean(dh * there, -1, keepdims=True))
        dx_o[at, :] = (dx + dy[at, :].astype(WIDE)).astype(LOW)

        @pl.when(n == 0)
        def _():
            for copy in sends:
                copy.start()

    lax.fori_loop(0, rows // step, second, None)
    got_s[0] = part_s[...]
    for copy in sends:
        copy.wait()
    dg_o[...] = sum(got_s[_slot(n, me, slots)] for n in range(slots)).sum(0, keepdims=True)


def finish(own, from_left, from_right, x, dy, gain, slots, step=64):
    rows, d = x.shape
    copies = pltpu.SemaphoreType.DMA((slots,))
    here = pl.BlockSpec(memory_space=pltpu.VMEM)
    return pl.pallas_call(
        functools.partial(_finish, slots=slots, step=step),
        in_specs=[here] * 6,
        out_specs=[here] * 2,
        out_shape=[_like((rows, d)), _like((1, d), WIDE)],
        scratch_shapes=[pltpu.VMEM((rows, d), WIDE), pltpu.VMEM((8, d), WIDE), pltpu.VMEM((slots, 8, d), WIDE), copies, copies],
        compiler_params=pltpu.CompilerParams(vmem_limit_bytes=24 * 2**20, collective_id=2, has_side_effects=True),
        cost_estimate=_cost(20 * rows * d, [own, own, x, x, x]),
        name="finish",
    )(own, x, dy, from_left, from_right, gain)


def solution(mesh):
    slots = mesh.shape["tp"]
    right = [(i, (i + 1) % slots) for i in range(slots)]
    left = [(i, (i - 1) % slots) for i in range(slots)]

    def step(x, dy, gain, wq, wk, wv, wo):
        rows, d = x.shape
        half = HEAD // 2
        pace = np.tile(np.float32(THETA) ** (-np.arange(half, dtype=np.float32) / half), 2)[None]
        _, dys, a, dqkv, o, to_right, to_left, own = front(x, dy, gain, pace, wq, wk, wv, wo, slots)
        from_left, from_right = lax.ppermute(to_right, "tp", right), lax.ppermute(to_left, "tp", left)
        later, o, _ = lax.optimization_barrier((dqkv, o, to_right))
        dy_all = dys.reshape(-1, d)
        by_w = [lax.dot_general(a, t, (((0,), (0,)), ((), ())), preferred_element_type=WIDE).astype(LOW) for t in jnp.split(later, 3, 1)]
        by_wo = lax.dot_general(o, dy_all, (((0,), (0,)), ((), ())), preferred_element_type=WIDE).astype(LOW)
        return (*finish(own, from_left, from_right, x, dy, gain[None], slots), *by_w, by_wo)

    tokens, columns = P(("dp", "tp"), None), P(None, "tp")
    return jax.shard_map(
        step,
        mesh=mesh,
        in_specs=(tokens, tokens, P(None), columns, columns, columns, P("tp", None)),
        out_specs=(tokens, P("dp", None), P("dp", "tp"), P("dp", "tp"), P("dp", "tp"), P(("dp", "tp"), None)),
        check_vma=False,
    )
```

```python
import functools

import jax
import jax.numpy as jnp
import numpy as np
from jax import lax
from jax.experimental import pallas as pl
from jax.experimental.pallas import tpu as pltpu
from jax.sharding import PartitionSpec as P

HEAD = 128
THETA = 10000
NEG = -1e30
HIDDEN = 2 * NEG
LOG2E = 1.4426950408889634
VMEM = 63 * 2**20
LOW = jnp.bfloat16
WIDE = jnp.float32


def _dot(a, b, ca, cb):
    return lax.dot_general(a, b, (((ca,), (cb,)), ((), ())), preferred_element_type=WIDE)


def _params(**more):
    return pltpu.CompilerParams(vmem_limit_bytes=VMEM, **more)


def _cost(flops, arrays, exps=0):
    return pl.CostEstimate(flops=int(flops), transcendentals=int(exps), bytes_accessed=int(sum(a.size * a.dtype.itemsize for a in arrays)))


def _like(shape, dtype=LOW):
    return jax.ShapeDtypeStruct(shape, dtype)


ANY = pl.BlockSpec(memory_space=pl.ANY)


def _full(shape):
    return pl.BlockSpec(shape, lambda *_: (0,) * len(shape))


def _turn(t, cos, sin):
    return t * cos + pltpu.roll(t, HEAD // 2, 1) * sin


def _slot(block, me, slots):
    return lax.rem(block - me + slots, slots)


def _gap(keys, queries):
    return lax.broadcasted_iota(jnp.int32, (keys, queries), 1) - lax.broadcasted_iota(jnp.int32, (keys, queries), 0)


def _front(x, dy, gain, pace, wq, wk, wv, wo, xs, dys, a_o, d_o, o_o, right_o, left_o, own_o,
           wo_s, x_s, a_s, qkv_s, o_s, do_s, lse_s, gap_s, cos, sin, got_s, w_sem, x_sem, a_sem, out_sem, term_sem, send_sem, recv_sem,
           *, slots, group):
    me = lax.axis_index("tp")
    rows, d = x.shape
    half, wide = rows // 2, wq.shape[1]
    heads = wide // HEAD
    right, left = lax.rem(me + 1, slots), lax.rem(me + slots - 1, slots)
    top, low = pl.ds(0, half), pl.ds(half, half)
    last = slots - 1
    scale = HEAD**-0.5
    e = scale * LOG2E

    barrier = pltpu.get_barrier_semaphore()
    for there in (left, right):
        pl.semaphore_signal(barrier, inc=1, device_id={"tp": there}, device_id_type=pl.DeviceIdType.MESH)
    pl.semaphore_wait(barrier, 2)

    def remote(n, src, dst, there):
        return pltpu.make_async_remote_copy(src_ref=src, dst_ref=dst, send_sem=send_sem.at[n], recv_sem=recv_sem.at[n],
                                            device_id={"tp": there}, device_id_type=pl.DeviceIdType.MESH)

    def transfers(n, t, ts):
        return [remote(n, t.at[top], ts.at[last, 0], right), remote(n + 1, t.at[low], ts.at[1, 1], left),
                remote(n + 2, t.at[low], ts.at[last, 1], right), remote(n + 3, t.at[top], ts.at[1, 0], left),
                remote(n + 4, ts.at[last, 0], ts.at[2, 0], right), remote(n + 5, ts.at[1, 1], ts.at[2, 1], left)]

    def start(copies):
        for copy in copies:
            copy.start()
        return copies

    def wait(copies):
        for copy in copies:
            copy.wait()

    def arrived(copies):
        for copy in copies:
            copy.wait_recv()

    x_go, dy_go = transfers(0, x, xs), transfers(6, dy, dys)
    start(x_go[:4])

    def into(ts, slot, p):
        return pltpu.make_async_copy(ts.at[slot, p], x_s.at[pl.ds(p * half, half)], x_sem.at[p])

    def own(t, p):
        return pltpu.make_async_copy(t.at[pl.ds(p * half, half)], x_s.at[pl.ds(p * half, half)], x_sem.at[p])

    def a_out(slot, p):
        return pltpu.make_async_copy(a_s.at[pl.ds(p * half, half)], a_o.at[pl.ds(slot * rows + p * half, half)], a_sem.at[p])

    loads = start([own(x, 0), own(x, 1)])
    wo_load = pltpu.make_async_copy(wo, wo_s, w_sem.at[3])
    gap_s[...] = _gap(rows, rows)

    def table(n, _):
        at = pl.ds(pl.multiple_of(n * 128, 128), 128)
        first = lax.rem(me + n * 128 // rows, slots) * rows + lax.rem(n * 128, rows)
        angle = (first + lax.broadcasted_iota(jnp.int32, (128, HEAD), 0)).astype(WIDE) * pace[...]
        cos[at, :] = jnp.cos(angle)
        sin[at, :] = jnp.where(lax.broadcasted_iota(jnp.int32, (128, HEAD), 1) < HEAD // 2, -1.0, 1.0) * jnp.sin(angle)

    lax.fori_loop(0, slots * rows // 128, table, None)
    g = gain[...].astype(WIDE).reshape(1, d)

    def by_seen(slot):
        at = slice(slot * rows, (slot + 1) * rows)

        for c in range(0, wide, 512):
            c = slice(c, min(c + 512, wide))
            do_s[at, c] = _dot(x_s[...], wo_s[c, :], 1, 1).astype(LOW)

    def head(n, h):
        return pl.ds(pl.multiple_of(n * wide + h * HEAD, HEAD), HEAD)

    def upward(w_s, top_s, mix_s):
        w_loads = start([pltpu.make_async_copy(w, w_s.at[:, pl.ds(i * wide, wide)], w_sem.at[i]) for i, w in enumerate((wq, wk, wv))])
        wo_load.start()
        top_s[...] = jnp.full_like(top_s, NEG)
        mix_s[...] = jnp.zeros_like(mix_s)

        def project(slot, parts, before):
            for p, earlier in zip(parts, before):
                if earlier is not None:
                    a_out(earlier, p).wait()
                for n in range(p * half, (p + 1) * half, 128):
                    t = x_s[n : n + 128, :].astype(WIDE)
                    size = lax.rsqrt(jnp.mean(t * t, -1, keepdims=True) + 1e-6)
                    a_s[n : n + 128, :] = (t * size * g).astype(LOW)
                a_out(slot, p).start()
            if slot == 0:
                wait(w_loads)
            first, count = parts[0] * half, len(parts) * half
            at, here = slice(slot * rows + first, slot * rows + first + count), slice(first, first + count)

            def turned(i, _):
                c = pl.ds(pl.multiple_of(i * 512, 512), 512)
                t = _dot(a_s[here, :], w_s[:, c], 1, 0).astype(LOW).astype(WIDE)
                qkv_s[at, c] = jnp.concatenate([_turn(t[:, h : h + HEAD], cos[at, :], sin[at, :]) for h in range(0, 512, HEAD)], 1).astype(LOW)

            lax.fori_loop(0, 2 * wide // 512, turned, None)
            for c in range(2 * wide, 3 * wide, 512):
                c = slice(c, min(c + 512, 3 * wide))
                qkv_s[at, c] = _dot(a_s[here, :], w_s[:, c], 1, 0).astype(LOW)

        def pair(sq, sk, masked, ks=(0, rows), qs=(0, rows)):
            mine, here = pl.ds(sq * rows + qs[0], qs[1] - qs[0]), pl.ds(sk * rows + ks[0], ks[1] - ks[0])
            to = slice(*qs)
            ones = jnp.ones((8, ks[1] - ks[0]), LOW)

            def some(k, _):
                hs = [k * group + h for h in range(group)]
                scores = [_dot(qkv_s[here, head(1, h)], qkv_s[mine, head(0, h)], 1, 1) for h in hs]
                weights, keeps = [], []
                for h, s in zip(hs, scores):
                    if masked:
                        s = jnp.where(gap_s[slice(*ks), to] >= 0, s, HIDDEN)
                    old = top_s[sq, pl.ds(h, 1), to]
                    most = jnp.maximum(old, s.max(axis=0, keepdims=True))
                    top_s[sq, pl.ds(h, 1), to] = most
                    weights.append(jnp.exp2((s - most) * e).astype(LOW))
                    keeps.append(jnp.exp2((old - most) * e))
                for h, p, keep in zip(hs, weights, keeps):
                    values = jnp.concatenate([qkv_s[here, head(2, h)].T, ones], axis=0)
                    mix_s[sq, h, :, to] = mix_s[sq, h, :, to] * keep + _dot(values, p, 1, 0)

            lax.fori_loop(0, heads // group, some, None)

        wait(loads)
        project(0, (0, 1), (None, None))
        wait(start([own(dy, 0), own(dy, 1)]))
        keep = start([pltpu.make_async_copy(x_s.at[pl.ds(p * half, half)], dys.at[0, p], x_sem.at[p]) for p in range(2)])
        wo_load.wait()
        by_seen(0)
        wait(keep)
        arrived(x_go[:2])
        start(x_go[4:])
        wait(start([into(xs, last, 0), into(xs, 1, 1)]))
        project(last, (0,), (0,))
        project(1, (1,), (0,))
        arrived(x_go[2:4])
        start(dy_go[:4])
        wait(start([into(xs, 1, 0), into(xs, last, 1)]))
        project(1, (0,), (last,))
        project(last, (1,), (1,))

        def step(n, _):
            @pl.when(n == 9)
            def _():
                arrived(x_go[4:])
                wait(start([into(xs, 2, 0), into(xs, 2, 1)]))
                project(2, (0, 1), (1, last))

            i, j = n // 3, n % 3
            m = n - 9
            sq = jnp.where(n < 9, i + i // 2, jnp.where(m < 4, 2, m - 4 + (m - 4) // 2))
            sk = jnp.where(n < 9, j + j // 2, jnp.where(m < 4, m, 2))
            bq, bk = lax.rem(me + sq, slots), lax.rem(me + sk, slots)

            @pl.when(bk < bq)
            def _():
                pair(sq, sk, False)

            @pl.when(bk == bq)
            def _():
                pair(sq, sk, True, ks=(0, half))
                pair(sq, sk, True, ks=(half, rows), qs=(half, rows))

        lax.fori_loop(0, slots * slots, step, None)

        def settle(slot, _):
            at = pl.ds(slot * rows, rows)
            for h in range(heads):
                total = mix_s[slot, h, HEAD : HEAD + 1, :]
                o_s[at, head(0, h)] = (mix_s[slot, h, :HEAD, :] * (1 / total)).T.astype(LOW)
                lse_s[slot, h : h + 1, :] = top_s[slot, h : h + 1, :] * e + jnp.log2(total)

        lax.fori_loop(0, slots, settle, None)
        wait([a_out(2, 0), a_out(2, 1)])

    pl.run_scoped(upward, pltpu.VMEM((d, 3 * wide), LOW), pltpu.VMEM((slots, heads, rows), WIDE),
                  pltpu.VMEM((slots, heads, HEAD + 8, rows), WIDE))
    o_out = start([pltpu.make_async_copy(o_s, o_o, w_sem.at[0])])
    arrived(dy_go[:2])
    start(dy_go[4:])

    def d_out(slot):
        at = pl.ds(slot * rows, rows)
        return pltpu.make_async_copy(qkv_s.at[at], d_o.at[at], out_sem.at[slot])

    def downward(w_s, dq_s, dk_s, dv_s):
        dk_s[...] = jnp.zeros_like(dk_s)
        dv_s[...] = jnp.zeros_like(dv_s)

        def step(n, _):
            @pl.when(n == 1)
            def _():
                arrived(dy_go[2:4])
                for slot in (1, last):
                    wait(start([into(dys, slot, 0), into(dys, slot, 1)]))
                    by_seen(slot)

            @pl.when(n == 3)
            def _():
                arrived(dy_go[4:])
                wait(start([into(dys, 2, 0), into(dys, 2, 1)]))
                by_seen(2)

            sq = jnp.where(n < 2, n, 5 - n)
            bq = lax.rem(me + sq, slots)
            mine = pl.ds(sq * rows, rows)

            def some(k, _):
                hs = [k * group + h for h in range(group)]
                cut = [head(0, h) for h in hs]
                dq_s[...] = jnp.zeros_like(dq_s)
                lses = [lse_s[sq, pl.ds(h, 1), :] for h in hs]
                deltas = [(do_s[mine, c].astype(WIDE) * o_s[mine, c].astype(WIDE)).T.sum(axis=0, keepdims=True) for c in cut]

                def block(j, masked, ks=(0, rows), qs=(0, rows)):
                    here = pl.ds(_slot(j, me, slots) * rows + ks[0], ks[1] - ks[0])
                    there, to = pl.ds(sq * rows + qs[0], qs[1] - qs[0]), slice(*qs)
                    scores = [_dot(qkv_s[here, head(1, h)], qkv_s[there, head(0, h)], 1, 1) for h in hs]
                    dps = [_dot(qkv_s[here, head(2, h)], do_s[there, c], 1, 1) for h, c in zip(hs, cut)]
                    for i, (h, c) in enumerate(zip(hs, cut)):
                        p = jnp.exp2(scores[i] * e - lses[i][:, to])
                        if masked:
                            p = jnp.where(gap_s[slice(*ks), to] >= 0, p, 0.0)
                        ds = (p * (dps[i] - deltas[i][:, to])).astype(LOW)
                        dv_s[here, c] += _dot(p.astype(LOW), do_s[there, c], 1, 0)
                        dk_s[here, c] += _dot(ds, qkv_s[there, c], 1, 0)
                        dq_s[i, :, to] += _dot(qkv_s[here, head(1, h)].T, ds, 1, 0)

                lax.fori_loop(0, bq, lambda j, _: block(j, False), None)
                block(bq, True, ks=(0, half))
                block(bq, True, ks=(half, rows), qs=(half, rows))
                for i, c in enumerate(cut):
                    dq = (dq_s[i] * scale).T.astype(LOW).astype(WIDE)
                    qkv_s[mine, c] = _turn(dq, cos[mine, :], -sin[mine, :]).astype(LOW)

            lax.fori_loop(0, heads // group, some, None)

        lax.fori_loop(0, slots, step, None)

        def settle(slot, _):
            at = pl.ds(slot * rows, rows)
            for h in range(heads):
                c = head(0, h)
                dk = (dk_s[at, c] * scale).astype(LOW).astype(WIDE)
                qkv_s[at, head(1, h)] = _turn(dk, cos[at, :], -sin[at, :]).astype(LOW)
                qkv_s[at, head(2, h)] = dv_s[at, c].astype(LOW)
            d_out(slot).start()

        settle(2, None)
        wait(w_in(w_s))

        def far(n, _):
            x_s[:, columns(n)] = term(w_s, 2, n).astype(LOW)
            for i in range(1, tiles):

                @pl.when(n == i)
                def _():
                    start(far_go[2 * i - 2 : 2 * i])

        def rest(n, _):
            settle(n + n // 2, None)

            @pl.when(n == 0)
            def _():
                start(far_go[2 * tiles - 2 :])

        lax.fori_loop(0, tiles, far, None)
        lax.fori_loop(0, slots - 1, rest, None)

    def across(w_s, low_s, wide_s, own_s):
        def near(n, _):
            part, one, two = pl.ds(pl.multiple_of(n * side, side), side), *(pl.ds(pl.multiple_of(n * tile + p * side, side), side) for p in range(2))
            t = term(w_s, 1, n)
            wide_s[0, :, part] = t[:, :side]
            low_s[0, :, two] = t[:, side:].astype(LOW)
            t = term(w_s, last, n)
            low_s[1, :, one] = t[:, :side].astype(LOW)
            wide_s[1, :, part] = t[:, side:]

        lax.fori_loop(0, tiles, near, None)

        def own(n, _):
            own_s[:, columns(n)] = term(w_s, 0, n)

        lax.fori_loop(0, tiles, own, None)
        own_out = start([pltpu.make_async_copy(own_s, own_o, term_sem.at[2])])
        for i, copy in enumerate(far_go):
            copy.wait_recv()
            n, p = i // 2, i % 2
            from_, to = slice(n * side, (n + 1) * side), slice(i * side, (i + 1) * side)

            def add(r, _):
                at = pl.ds(pl.multiple_of(r * 256, 256), 256)
                low_s[p, at, to] = (wide_s[p, at, from_] + got_s[i, at, :].astype(WIDE)).astype(LOW)

            lax.fori_loop(0, rows // 256, add, None)
        wait(start([pltpu.make_async_copy(low_s.at[p], o, term_sem.at[p]) for p, o in enumerate((right_o, left_o))]))
        wait(own_out)

    tiles, tile, side = 4, d // 4, d // 8
    far_go = [remote(12 + i, x_s.at[:, pl.ds(i * side, side)], got_s.at[i], (right, left)[i % 2]) for i in range(2 * tiles)]

    def columns(n):
        return pl.ds(pl.multiple_of(n * tile, tile), tile)

    def term(w_s, slot, n):
        return _dot(qkv_s[slot * rows : (slot + 1) * rows, :], w_s[columns(n), :], 1, 1)

    def w_in(w_s):
        return [pltpu.make_async_copy(w, w_s.at[:, pl.ds(i * wide, wide)], w_sem.at[1 + i]) for i, w in enumerate((wq, wk, wv))]

    def downward_and_across(w_s):
        start(w_in(w_s))
        pl.run_scoped(functools.partial(downward, w_s), pltpu.VMEM((group, HEAD, rows), WIDE), pltpu.VMEM((slots * rows, wide), WIDE),
                      pltpu.VMEM((slots * rows, wide), WIDE))
        pl.run_scoped(functools.partial(across, w_s), pltpu.VMEM((2, rows, d), LOW), pltpu.VMEM((2, rows, d // 2), WIDE),
                      pltpu.VMEM((rows, d), WIDE))

    pl.run_scoped(downward_and_across, pltpu.VMEM((d, 3 * wide), LOW))
    wait(o_out)
    wait([d_out(slot) for slot in range(slots)])
    for copy in (*x_go, *dy_go, *far_go):
        copy.wait_send()


def front(x, dy, gain, pace, wq, wk, wv, wo, slots, group=3):
    rows, d = x.shape
    wide = wq.shape[1]
    total, heads = slots * rows, wide // HEAD
    blocks = _like((slots, 2, rows // 2, d))
    copies = pltpu.SemaphoreType.DMA((20,))
    return pl.pallas_call(
        functools.partial(_front, slots=slots, group=group),
        in_specs=[ANY, ANY] + [pl.BlockSpec(memory_space=pltpu.VMEM)] * 2 + [ANY] * 4,
        out_specs=[ANY] * 8,
        out_shape=[blocks, blocks, _like((total, d)), _like((total, 3 * wide)), _like((total, wide)), _like((rows, d)), _like((rows, d)),
                   _like((rows, d), WIDE)],
        scratch_shapes=[pltpu.VMEM((wide, d), LOW), pltpu.VMEM((rows, d), LOW), pltpu.VMEM((rows, d), LOW),
                        pltpu.VMEM((total, 3 * wide), LOW), pltpu.VMEM((total, wide), LOW), pltpu.VMEM((total, wide), LOW),
                        pltpu.VMEM((slots, heads, rows), WIDE), pltpu.VMEM((rows, rows), jnp.int32),
                        pltpu.VMEM((total, HEAD), WIDE), pltpu.VMEM((total, HEAD), WIDE), pltpu.VMEM((8, rows, d // 8), LOW),
                        pltpu.SemaphoreType.DMA((4,)), pltpu.SemaphoreType.DMA((2,)), pltpu.SemaphoreType.DMA((2,)),
                        pltpu.SemaphoreType.DMA((slots,)), pltpu.SemaphoreType.DMA((3,)), copies, copies],
        compiler_params=_params(collective_id=0, has_side_effects=True),
        cost_estimate=_cost(2 * total * d * 7 * wide + 14 * total * total * wide, [x] * 20, 2 * total * total * heads),
        name="front",
    )(x, dy, gain, pace, wq, wk, wv, wo)


def _finish(own, x, dy, from_left, from_right, gain, dx_o, dg_o, dn_s, part_s, got_s, send_sem, recv_sem, *, slots, step):
    me = lax.axis_index("tp")
    rows, d = x.shape
    others = [lax.rem(me + s, slots) for s in range(1, slots)]
    barrier = pltpu.get_barrier_semaphore()
    for there in others:
        pl.semaphore_signal(barrier, inc=1, device_id={"tp": there}, device_id_type=pl.DeviceIdType.MESH)
    g = gain[...].astype(WIDE)
    part_s[...] = jnp.zeros_like(part_s)

    def first(n, _):
        at = pl.ds(pl.multiple_of(n * step, step), step)
        t = x[at, :].astype(WIDE)
        dn = own[at, :] + from_left[at, :].astype(WIDE) + from_right[at, :].astype(WIDE)
        dn_s[at, :] = dn
        part_s[...] += (dn * (t * lax.rsqrt(jnp.mean(t * t, -1, keepdims=True) + 1e-6))).reshape(-1, 8, d).sum(0)

    lax.fori_loop(0, rows // step, first, None)
    pl.semaphore_wait(barrier, slots - 1)
    sends = [pltpu.make_async_remote_copy(src_ref=part_s, dst_ref=got_s.at[slots - s], send_sem=send_sem.at[s], recv_sem=recv_sem.at[s],
                                          device_id={"tp": there}, device_id_type=pl.DeviceIdType.MESH) for s, there in enumerate(others, 1)]

    def second(n, _):
        at = pl.ds(pl.multiple_of(n * step, step), step)
        t = x[at, :].astype(WIDE)
        size = lax.rsqrt(jnp.mean(t * t, -1, keepdims=True) + 1e-6)
        there = t * size
        dh = dn_s[at, :] * g
        dx = size * (dh - there * jnp.mean(dh * there, -1, keepdims=True))
        dx_o[at, :] = (dx + dy[at, :].astype(WIDE)).astype(LOW)

        @pl.when(n == 0)
        def _():
            for copy in sends:
                copy.start()

    lax.fori_loop(0, rows // step, second, None)
    got_s[0] = part_s[...]
    for copy in sends:
        copy.wait()
    dg_o[...] = sum(got_s[_slot(n, me, slots)] for n in range(slots)).sum(0, keepdims=True)


def finish(own, from_left, from_right, x, dy, gain, slots, step=64):
    rows, d = x.shape
    copies = pltpu.SemaphoreType.DMA((slots,))
    here = pl.BlockSpec(memory_space=pltpu.VMEM)
    return pl.pallas_call(
        functools.partial(_finish, slots=slots, step=step),
        in_specs=[here] * 6,
        out_specs=[here] * 2,
        out_shape=[_like((rows, d)), _like((1, d), WIDE)],
        scratch_shapes=[pltpu.VMEM((rows, d), WIDE), pltpu.VMEM((8, d), WIDE), pltpu.VMEM((slots, 8, d), WIDE), copies, copies],
        compiler_params=pltpu.CompilerParams(vmem_limit_bytes=24 * 2**20, collective_id=2, has_side_effects=True),
        cost_estimate=_cost(20 * rows * d, [own, own, x, x, x]),
        name="finish",
    )(own, x, dy, from_left, from_right, gain)


def solution(mesh):
    slots = mesh.shape["tp"]
    right = [(i, (i + 1) % slots) for i in range(slots)]
    left = [(i, (i - 1) % slots) for i in range(slots)]

    def step(x, dy, gain, wq, wk, wv, wo):
        rows, d = x.shape
        half = HEAD // 2
        pace = np.tile(np.float32(THETA) ** (-np.arange(half, dtype=np.float32) / half), 2)[None]
        _, dys, a, dqkv, o, to_right, to_left, own = front(x, dy, gain, pace, wq, wk, wv, wo, slots)
        from_left, from_right = lax.ppermute(to_right, "tp", right), lax.ppermute(to_left, "tp", left)
        later, o, _ = lax.optimization_barrier((dqkv, o, to_right))
        dy_all = dys.reshape(-1, d)
        by_w = [lax.dot_general(a, t, (((0,), (0,)), ((), ())), preferred_element_type=WIDE).astype(LOW) for t in jnp.split(later, 3, 1)]
        by_wo = lax.dot_general(o, dy_all, (((0,), (0,)), ((), ())), preferred_element_type=WIDE).astype(LOW)
        return (*finish(own, from_left, from_right, x, dy, gain[None], slots), *by_w, by_wo)

    tokens, columns = P(("dp", "tp"), None), P(None, "tp")
    return jax.shard_map(
        step,
        mesh=mesh,
        in_specs=(tokens, tokens, P(None), columns, columns, columns, P("tp", None)),
        out_specs=(tokens, P("dp", None), P("dp", "tp"), P("dp", "tp"), P("dp", "tp"), P(("dp", "tp"), None)),
        check_vma=False,
    )
```

```python
import functools

import jax
import jax.numpy as jnp
import numpy as np
from jax import lax
from jax.experimental import pallas as pl
from jax.experimental.pallas import tpu as pltpu
from jax.sharding import PartitionSpec as P

HEAD = 128
THETA = 10000
NEG = -1e30
HIDDEN = 2 * NEG
LOG2E = 1.4426950408889634
VMEM = 63 * 2**20
LOW = jnp.bfloat16
WIDE = jnp.float32


def _dot(a, b, ca, cb):
    return lax.dot_general(a, b, (((ca,), (cb,)), ((), ())), preferred_element_type=WIDE)


def _params(**more):
    return pltpu.CompilerParams(vmem_limit_bytes=VMEM, **more)


def _cost(flops, arrays, exps=0):
    return pl.CostEstimate(flops=int(flops), transcendentals=int(exps), bytes_accessed=int(sum(a.size * a.dtype.itemsize for a in arrays)))


def _like(shape, dtype=LOW):
    return jax.ShapeDtypeStruct(shape, dtype)


ANY = pl.BlockSpec(memory_space=pl.ANY)


def _full(shape):
    return pl.BlockSpec(shape, lambda *_: (0,) * len(shape))


def _turn(t, cos, sin):
    return t * cos + pltpu.roll(t, HEAD // 2, 1) * sin


def _slot(block, me, slots):
    return lax.rem(block - me + slots, slots)


def _gap(keys, queries):
    return lax.broadcasted_iota(jnp.int32, (keys, queries), 1) - lax.broadcasted_iota(jnp.int32, (keys, queries), 0)


def _front(x, dy, gain, pace, wq, wk, wv, wo, xs, dys, a_o, d_o, o_o, right_o, left_o, own_o,
           wo_s, x_s, a_s, qkv_s, o_s, do_s, lse_s, gap_s, cos, sin, got_s, w_sem, x_sem, a_sem, out_sem, term_sem, send_sem, recv_sem,
           *, slots, group):
    me = lax.axis_index("tp")
    rows, d = x.shape
    half, wide = rows // 2, wq.shape[1]
    heads = wide // HEAD
    right, left = lax.rem(me + 1, slots), lax.rem(me + slots - 1, slots)
    top, low = pl.ds(0, half), pl.ds(half, half)
    last = slots - 1
    scale = HEAD**-0.5
    e = scale * LOG2E

    barrier = pltpu.get_barrier_semaphore()
    for there in (left, right):
        pl.semaphore_signal(barrier, inc=1, device_id={"tp": there}, device_id_type=pl.DeviceIdType.MESH)
    pl.semaphore_wait(barrier, 2)

    def remote(n, src, dst, there):
        return pltpu.make_async_remote_copy(src_ref=src, dst_ref=dst, send_sem=send_sem.at[n], recv_sem=recv_sem.at[n],
                                            device_id={"tp": there}, device_id_type=pl.DeviceIdType.MESH)

    def transfers(n, t, ts):
        return [remote(n, t.at[top], ts.at[last, 0], right), remote(n + 1, t.at[low], ts.at[1, 1], left),
                remote(n + 2, t.at[low], ts.at[last, 1], right), remote(n + 3, t.at[top], ts.at[1, 0], left),
                remote(n + 4, ts.at[last, 0], ts.at[2, 0], right), remote(n + 5, ts.at[1, 1], ts.at[2, 1], left)]

    def start(copies):
        for copy in copies:
            copy.start()
        return copies

    def wait(copies):
        for copy in copies:
            copy.wait()

    def arrived(copies):
        for copy in copies:
            copy.wait_recv()

    x_go, dy_go = transfers(0, x, xs), transfers(6, dy, dys)
    start(x_go[:4])

    def into(ts, slot, p):
        return pltpu.make_async_copy(ts.at[slot, p], x_s.at[pl.ds(p * half, half)], x_sem.at[p])

    def own(t, p):
        return pltpu.make_async_copy(t.at[pl.ds(p * half, half)], x_s.at[pl.ds(p * half, half)], x_sem.at[p])

    def a_out(slot, p):
        return pltpu.make_async_copy(a_s.at[pl.ds(p * half, half)], a_o.at[pl.ds(slot * rows + p * half, half)], a_sem.at[p])

    loads = start([own(x, 0), own(x, 1)])
    wo_load = pltpu.make_async_copy(wo, wo_s, w_sem.at[3])
    gap_s[...] = _gap(rows, rows)

    def table(n, _):
        at = pl.ds(pl.multiple_of(n * 128, 128), 128)
        first = lax.rem(me + n * 128 // rows, slots) * rows + lax.rem(n * 128, rows)
        angle = (first + lax.broadcasted_iota(jnp.int32, (128, HEAD), 0)).astype(WIDE) * pace[...]
        cos[at, :] = jnp.cos(angle)
        sin[at, :] = jnp.where(lax.broadcasted_iota(jnp.int32, (128, HEAD), 1) < HEAD // 2, -1.0, 1.0) * jnp.sin(angle)

    lax.fori_loop(0, slots * rows // 128, table, None)
    g = gain[...].astype(WIDE).reshape(1, d)

    def by_seen(slot):
        at = slice(slot * rows, (slot + 1) * rows)

        for c in range(0, wide, 512):
            c = slice(c, min(c + 512, wide))
            do_s[at, c] = _dot(x_s[...], wo_s[c, :], 1, 1).astype(LOW)

    def head(n, h):
        return pl.ds(pl.multiple_of(n * wide + h * HEAD, HEAD), HEAD)

    def upward(w_s, top_s, mix_s):
        w_loads = start([pltpu.make_async_copy(w, w_s.at[:, pl.ds(i * wide, wide)], w_sem.at[i]) for i, w in enumerate((wq, wk, wv))])
        wo_load.start()
        top_s[...] = jnp.full_like(top_s, NEG)
        mix_s[...] = jnp.zeros_like(mix_s)

        def project(slot, parts, before):
            for p, earlier in zip(parts, before):
                if earlier is not None:
                    a_out(earlier, p).wait()
                for n in range(p * half, (p + 1) * half, 128):
                    t = x_s[n : n + 128, :].astype(WIDE)
                    size = lax.rsqrt(jnp.mean(t * t, -1, keepdims=True) + 1e-6)
                    a_s[n : n + 128, :] = (t * size * g).astype(LOW)
                a_out(slot, p).start()
            if slot == 0:
                wait(w_loads)
            first, count = parts[0] * half, len(parts) * half
            at, here = slice(slot * rows + first, slot * rows + first + count), slice(first, first + count)

            def turned(i, _):
                c = pl.ds(pl.multiple_of(i * 512, 512), 512)
                t = _dot(a_s[here, :], w_s[:, c], 1, 0).astype(LOW).astype(WIDE)
                qkv_s[at, c] = jnp.concatenate([_turn(t[:, h : h + HEAD], cos[at, :], sin[at, :]) for h in range(0, 512, HEAD)], 1).astype(LOW)

            lax.fori_loop(0, 2 * wide // 512, turned, None)
            for c in range(2 * wide, 3 * wide, 512):
                c = slice(c, min(c + 512, 3 * wide))
                qkv_s[at, c] = _dot(a_s[here, :], w_s[:, c], 1, 0).astype(LOW)

        def pair(sq, sk, masked, ks=(0, rows), qs=(0, rows)):
            mine, here = pl.ds(sq * rows + qs[0], qs[1] - qs[0]), pl.ds(sk * rows + ks[0], ks[1] - ks[0])
            to = slice(*qs)
            ones = jnp.ones((8, ks[1] - ks[0]), LOW)

            def some(k, _):
                hs = [k * group + h for h in range(group)]
                scores = [_dot(qkv_s[here, head(1, h)], qkv_s[mine, head(0, h)], 1, 1) for h in hs]
                weights, keeps = [], []
                for h, s in zip(hs, scores):
                    if masked:
                        s = jnp.where(gap_s[slice(*ks), to] >= 0, s, HIDDEN)
                    old = top_s[sq, pl.ds(h, 1), to]
                    most = jnp.maximum(old, s.max(axis=0, keepdims=True))
                    top_s[sq, pl.ds(h, 1), to] = most
                    weights.append(jnp.exp2((s - most) * e).astype(LOW))
                    keeps.append(jnp.exp2((old - most) * e))
                for h, p, keep in zip(hs, weights, keeps):
                    values = jnp.concatenate([qkv_s[here, head(2, h)].T, ones], axis=0)
                    mix_s[sq, h, :, to] = mix_s[sq, h, :, to] * keep + _dot(values, p, 1, 0)

            lax.fori_loop(0, heads // group, some, None)

        wait(loads)
        project(0, (0, 1), (None, None))
        wait(start([own(dy, 0), own(dy, 1)]))
        keep = start([pltpu.make_async_copy(x_s.at[pl.ds(p * half, half)], dys.at[0, p], x_sem.at[p]) for p in range(2)])
        wo_load.wait()
        by_seen(0)
        wait(keep)
        arrived(x_go[:2])
        start(x_go[4:])
        wait(start([into(xs, last, 0), into(xs, 1, 1)]))
        project(last, (0,), (0,))
        project(1, (1,), (0,))
        arrived(x_go[2:4])
        start(dy_go[:4])
        wait(start([into(xs, 1, 0), into(xs, last, 1)]))
        project(1, (0,), (last,))
        project(last, (1,), (1,))

        def step(n, _):
            @pl.when(n == 9)
            def _():
                arrived(x_go[4:])
                wait(start([into(xs, 2, 0), into(xs, 2, 1)]))
                project(2, (0, 1), (1, last))

            i, j = n // 3, n % 3
            m = n - 9
            sq = jnp.where(n < 9, i + i // 2, jnp.where(m < 4, 2, m - 4 + (m - 4) // 2))
            sk = jnp.where(n < 9, j + j // 2, jnp.where(m < 4, m, 2))
            bq, bk = lax.rem(me + sq, slots), lax.rem(me + sk, slots)

            @pl.when(bk < bq)
            def _():
                pair(sq, sk, False)

            @pl.when(bk == bq)
            def _():
                pair(sq, sk, True, ks=(0, half))
                pair(sq, sk, True, ks=(half, rows), qs=(half, rows))

        lax.fori_loop(0, slots * slots, step, None)

        def settle(slot, _):
            at = pl.ds(slot * rows, rows)
            for h in range(heads):
                total = mix_s[slot, h, HEAD : HEAD + 1, :]
                o_s[at, head(0, h)] = (mix_s[slot, h, :HEAD, :] * (1 / total)).T.astype(LOW)
                lse_s[slot, h : h + 1, :] = top_s[slot, h : h + 1, :] * e + jnp.log2(total)

        lax.fori_loop(0, slots, settle, None)
        wait([a_out(2, 0), a_out(2, 1)])

    pl.run_scoped(upward, pltpu.VMEM((d, 3 * wide), LOW), pltpu.VMEM((slots, heads, rows), WIDE),
                  pltpu.VMEM((slots, heads, HEAD + 8, rows), WIDE))
    o_out = start([pltpu.make_async_copy(o_s, o_o, w_sem.at[0])])
    arrived(dy_go[:2])
    start(dy_go[4:])

    def d_out(slot):
        at = pl.ds(slot * rows, rows)
        return pltpu.make_async_copy(qkv_s.at[at], d_o.at[at], out_sem.at[slot])

    def downward(w_s, dq_s, dk_s, dv_s):
        dk_s[...] = jnp.zeros_like(dk_s)
        dv_s[...] = jnp.zeros_like(dv_s)

        def step(n, _):
            @pl.when(n == 1)
            def _():
                arrived(dy_go[2:4])
                for slot in (1, last):
                    wait(start([into(dys, slot, 0), into(dys, slot, 1)]))
                    by_seen(slot)

            @pl.when(n == 3)
            def _():
                arrived(dy_go[4:])
                wait(start([into(dys, 2, 0), into(dys, 2, 1)]))
                by_seen(2)

            sq = jnp.where(n < 2, n, 5 - n)
            bq = lax.rem(me + sq, slots)
            mine = pl.ds(sq * rows, rows)

            def some(k, _):
                hs = [k * group + h for h in range(group)]
                cut = [head(0, h) for h in hs]
                dq_s[...] = jnp.zeros_like(dq_s)
                lses = [lse_s[sq, pl.ds(h, 1), :] for h in hs]
                deltas = [(do_s[mine, c].astype(WIDE) * o_s[mine, c].astype(WIDE)).T.sum(axis=0, keepdims=True) for c in cut]

                def block(j, masked, ks=(0, rows), qs=(0, rows)):
                    here = pl.ds(_slot(j, me, slots) * rows + ks[0], ks[1] - ks[0])
                    there, to = pl.ds(sq * rows + qs[0], qs[1] - qs[0]), slice(*qs)
                    scores = [_dot(qkv_s[here, head(1, h)], qkv_s[there, head(0, h)], 1, 1) for h in hs]
                    dps = [_dot(qkv_s[here, head(2, h)], do_s[there, c], 1, 1) for h, c in zip(hs, cut)]
                    for i, (h, c) in enumerate(zip(hs, cut)):
                        p = jnp.exp2(scores[i] * e - lses[i][:, to])
                        if masked:
                            p = jnp.where(gap_s[slice(*ks), to] >= 0, p, 0.0)
                        ds = (p * (dps[i] - deltas[i][:, to])).astype(LOW)
                        dv_s[here, c] += _dot(p.astype(LOW), do_s[there, c], 1, 0)
                        dk_s[here, c] += _dot(ds, qkv_s[there, c], 1, 0)
                        dq_s[i, :, to] += _dot(qkv_s[here, head(1, h)].T, ds, 1, 0)

                lax.fori_loop(0, bq, lambda j, _: block(j, False), None)
                block(bq, True, ks=(0, half))
                block(bq, True, ks=(half, rows), qs=(half, rows))
                for i, c in enumerate(cut):
                    dq = (dq_s[i] * scale).T.astype(LOW).astype(WIDE)
                    qkv_s[mine, c] = _turn(dq, cos[mine, :], -sin[mine, :]).astype(LOW)

            lax.fori_loop(0, heads // group, some, None)

        lax.fori_loop(0, slots, step, None)

        def settle(slot, _):
            at = pl.ds(slot * rows, rows)
            for h in range(heads):
                c = head(0, h)
                dk = (dk_s[at, c] * scale).astype(LOW).astype(WIDE)
                qkv_s[at, head(1, h)] = _turn(dk, cos[at, :], -sin[at, :]).astype(LOW)
                qkv_s[at, head(2, h)] = dv_s[at, c].astype(LOW)
            d_out(slot).start()

        settle(2, None)
        wait(w_in(w_s))

        def far(n, _):
            x_s[:, columns(n)] = term(w_s, 2, n).astype(LOW)
            for i in range(1, tiles):

                @pl.when(n == i)
                def _():
                    start(far_go[2 * i - 2 : 2 * i])

        def rest(n, _):
            settle(n + n // 2, None)

            @pl.when(n == 0)
            def _():
                start(far_go[2 * tiles - 2 :])

        lax.fori_loop(0, tiles, far, None)
        lax.fori_loop(0, slots - 1, rest, None)

    def across(w_s, low_s, wide_s, own_s):
        def near(n, _):
            part, one, two = pl.ds(pl.multiple_of(n * side, side), side), *(pl.ds(pl.multiple_of(n * tile + p * side, side), side) for p in range(2))
            t = term(w_s, 1, n)
            wide_s[0, :, part] = t[:, :side]
            low_s[0, :, two] = t[:, side:].astype(LOW)
            t = term(w_s, last, n)
            low_s[1, :, one] = t[:, :side].astype(LOW)
            wide_s[1, :, part] = t[:, side:]

        lax.fori_loop(0, tiles, near, None)

        def own(n, _):
            own_s[:, columns(n)] = term(w_s, 0, n)

        lax.fori_loop(0, tiles, own, None)
        own_out = start([pltpu.make_async_copy(own_s, own_o, term_sem.at[0])])

        def out(p, i):
            at = pl.ds(i * side, side)
            return pltpu.make_async_copy(low_s.at[p, :, at], (right_o, left_o)[p].at[:, at], term_sem.at[1 + p * 2 * tiles + i])

        outs = start([out(1 - i % 2, i) for i in range(2 * tiles)])
        for i, copy in enumerate(far_go):
            copy.wait_recv()
            n, p = i // 2, i % 2
            from_, to = slice(n * side, (n + 1) * side), slice(i * side, (i + 1) * side)

            def add(r, _):
                at = pl.ds(pl.multiple_of(r * 256, 256), 256)
                low_s[p, at, to] = (wide_s[p, at, from_] + got_s[i, at, :].astype(WIDE)).astype(LOW)

            lax.fori_loop(0, rows // 256, add, None)
            outs += start([out(p, i)])
        wait(outs)
        wait(own_out)

    tiles, tile, side = 4, d // 4, d // 8
    far_go = [remote(12 + i, x_s.at[:, pl.ds(i * side, side)], got_s.at[i], (right, left)[i % 2]) for i in range(2 * tiles)]

    def columns(n):
        return pl.ds(pl.multiple_of(n * tile, tile), tile)

    def term(w_s, slot, n):
        return _dot(qkv_s[slot * rows : (slot + 1) * rows, :], w_s[columns(n), :], 1, 1)

    def w_in(w_s):
        return [pltpu.make_async_copy(w, w_s.at[:, pl.ds(i * wide, wide)], w_sem.at[1 + i]) for i, w in enumerate((wq, wk, wv))]

    def downward_and_across(w_s):
        start(w_in(w_s))
        pl.run_scoped(functools.partial(downward, w_s), pltpu.VMEM((group, HEAD, rows), WIDE), pltpu.VMEM((slots * rows, wide), WIDE),
                      pltpu.VMEM((slots * rows, wide), WIDE))
        pl.run_scoped(functools.partial(across, w_s), pltpu.VMEM((2, rows, d), LOW), pltpu.VMEM((2, rows, d // 2), WIDE),
                      pltpu.VMEM((rows, d), WIDE))

    pl.run_scoped(downward_and_across, pltpu.VMEM((d, 3 * wide), LOW))
    wait(o_out)
    wait([d_out(slot) for slot in range(slots)])
    for copy in (*x_go, *dy_go, *far_go):
        copy.wait_send()


def front(x, dy, gain, pace, wq, wk, wv, wo, slots, group=3):
    rows, d = x.shape
    wide = wq.shape[1]
    total, heads = slots * rows, wide // HEAD
    blocks = _like((slots, 2, rows // 2, d))
    copies = pltpu.SemaphoreType.DMA((20,))
    return pl.pallas_call(
        functools.partial(_front, slots=slots, group=group),
        in_specs=[ANY, ANY] + [pl.BlockSpec(memory_space=pltpu.VMEM)] * 2 + [ANY] * 4,
        out_specs=[ANY] * 8,
        out_shape=[blocks, blocks, _like((total, d)), _like((total, 3 * wide)), _like((total, wide)), _like((rows, d)), _like((rows, d)),
                   _like((rows, d), WIDE)],
        scratch_shapes=[pltpu.VMEM((wide, d), LOW), pltpu.VMEM((rows, d), LOW), pltpu.VMEM((rows, d), LOW),
                        pltpu.VMEM((total, 3 * wide), LOW), pltpu.VMEM((total, wide), LOW), pltpu.VMEM((total, wide), LOW),
                        pltpu.VMEM((slots, heads, rows), WIDE), pltpu.VMEM((rows, rows), jnp.int32),
                        pltpu.VMEM((total, HEAD), WIDE), pltpu.VMEM((total, HEAD), WIDE), pltpu.VMEM((8, rows, d // 8), LOW),
                        pltpu.SemaphoreType.DMA((4,)), pltpu.SemaphoreType.DMA((2,)), pltpu.SemaphoreType.DMA((2,)),
                        pltpu.SemaphoreType.DMA((slots,)), pltpu.SemaphoreType.DMA((17,)), copies, copies],
        compiler_params=_params(collective_id=0, has_side_effects=True),
        cost_estimate=_cost(2 * total * d * 7 * wide + 14 * total * total * wide, [x] * 20, 2 * total * total * heads),
        name="front",
    )(x, dy, gain, pace, wq, wk, wv, wo)


def _finish(own, x, dy, from_left, from_right, gain, dx_o, dg_o, dn_s, part_s, got_s, send_sem, recv_sem, *, slots, step):
    me = lax.axis_index("tp")
    rows, d = x.shape
    others = [lax.rem(me + s, slots) for s in range(1, slots)]
    barrier = pltpu.get_barrier_semaphore()
    for there in others:
        pl.semaphore_signal(barrier, inc=1, device_id={"tp": there}, device_id_type=pl.DeviceIdType.MESH)
    g = gain[...].astype(WIDE)
    part_s[...] = jnp.zeros_like(part_s)

    def first(n, _):
        at = pl.ds(pl.multiple_of(n * step, step), step)
        t = x[at, :].astype(WIDE)
        dn = own[at, :] + from_left[at, :].astype(WIDE) + from_right[at, :].astype(WIDE)
        dn_s[at, :] = dn
        part_s[...] += (dn * (t * lax.rsqrt(jnp.mean(t * t, -1, keepdims=True) + 1e-6))).reshape(-1, 8, d).sum(0)

    lax.fori_loop(0, rows // step, first, None)
    pl.semaphore_wait(barrier, slots - 1)
    sends = [pltpu.make_async_remote_copy(src_ref=part_s, dst_ref=got_s.at[slots - s], send_sem=send_sem.at[s], recv_sem=recv_sem.at[s],
                                          device_id={"tp": there}, device_id_type=pl.DeviceIdType.MESH) for s, there in enumerate(others, 1)]

    def second(n, _):
        at = pl.ds(pl.multiple_of(n * step, step), step)
        t = x[at, :].astype(WIDE)
        size = lax.rsqrt(jnp.mean(t * t, -1, keepdims=True) + 1e-6)
        there = t * size
        dh = dn_s[at, :] * g
        dx = size * (dh - there * jnp.mean(dh * there, -1, keepdims=True))
        dx_o[at, :] = (dx + dy[at, :].astype(WIDE)).astype(LOW)

        @pl.when(n == 0)
        def _():
            for copy in sends:
                copy.start()

    lax.fori_loop(0, rows // step, second, None)
    got_s[0] = part_s[...]
    for copy in sends:
        copy.wait()
    dg_o[...] = sum(got_s[_slot(n, me, slots)] for n in range(slots)).sum(0, keepdims=True)


def finish(own, from_left, from_right, x, dy, gain, slots, step=128):
    rows, d = x.shape
    copies = pltpu.SemaphoreType.DMA((slots,))
    here = pl.BlockSpec(memory_space=pltpu.VMEM)
    return pl.pallas_call(
        functools.partial(_finish, slots=slots, step=step),
        in_specs=[here] * 6,
        out_specs=[here] * 2,
        out_shape=[_like((rows, d)), _like((1, d), WIDE)],
        scratch_shapes=[pltpu.VMEM((rows, d), WIDE), pltpu.VMEM((8, d), WIDE), pltpu.VMEM((slots, 8, d), WIDE), copies, copies],
        compiler_params=pltpu.CompilerParams(vmem_limit_bytes=24 * 2**20, collective_id=2, has_side_effects=True),
        cost_estimate=_cost(20 * rows * d, [own, own, x, x, x]),
        name="finish",
    )(own, x, dy, from_left, from_right, gain)


def solution(mesh):
    slots = mesh.shape["tp"]
    right = [(i, (i + 1) % slots) for i in range(slots)]
    left = [(i, (i - 1) % slots) for i in range(slots)]

    def step(x, dy, gain, wq, wk, wv, wo):
        rows, d = x.shape
        half = HEAD // 2
        pace = np.tile(np.float32(THETA) ** (-np.arange(half, dtype=np.float32) / half), 2)[None]
        _, dys, a, dqkv, o, to_right, to_left, own = front(x, dy, gain, pace, wq, wk, wv, wo, slots)
        from_left, from_right = lax.ppermute(to_right, "tp", right), lax.ppermute(to_left, "tp", left)
        later, o, _ = lax.optimization_barrier((dqkv, o, to_right))
        dy_all = dys.reshape(-1, d)
        by_w = [lax.dot_general(a, t, (((0,), (0,)), ((), ())), preferred_element_type=WIDE).astype(LOW) for t in jnp.split(later, 3, 1)]
        by_wo = lax.dot_general(o, dy_all, (((0,), (0,)), ((), ())), preferred_element_type=WIDE).astype(LOW)
        return (*finish(own, from_left, from_right, x, dy, gain[None], slots), *by_w, by_wo)

    tokens, columns = P(("dp", "tp"), None), P(None, "tp")
    return jax.shard_map(
        step,
        mesh=mesh,
        in_specs=(tokens, tokens, P(None), columns, columns, columns, P("tp", None)),
        out_specs=(tokens, P("dp", None), P("dp", "tp"), P("dp", "tp"), P("dp", "tp"), P(("dp", "tp"), None)),
        check_vma=False,
    )
```
